128 devices in a mesh: head: 8 (over y, core), row: 16 (over x, z).
Axes of the slice: x: 4, y: 4, z: 4, core: 2. Of those that a mesh axis runs over, the one named last changes fastest.
Arguments:
- hidden_in: bfloat16 [512, 2048], replicated, may hold values from -6 to 6
- w_query: bfloat16 [2048, 16, 128], P(None, 'head', 'row'), may hold values from -0.125 to 0.125
- w_key: bfloat16 [2048, 16, 128], P(None, 'head', 'row'), may hold values from -0.125 to 0.125
- w_value: bfloat16 [2048, 32, 128], P(None, 'head'), may hold values from -0.125 to 0.125
- w_zgate: bfloat16 [2048, 32, 128], P(None, 'head'), may hold values from -0.125 to 0.125
- w_decay: bfloat16 [2048, 32], P(None, 'head'), may hold values from -0.125 to 0.125
- w_beta: bfloat16 [2048, 32], P(None, 'head'), may hold values from -0.125 to 0.125
- decay_log: float32 [32], P('head'), may hold values from -1.5 to 1.5
- dt_bias: float32 [32], P('head'), may hold values from -2 to 2
- norm_gain: float32 [128], replicated, may hold values from 0.1 to 1.9
- w_out: bfloat16 [32, 128, 2048], P('head'), may hold values from -0.09375 to 0.09375
- state: float32 [512, 32, 128, 128], P(None, 'head', 'row'), may hold values from -6 to 6
Outputs:
- layer_out: bfloat16 [512, 2048], P('row', 'head')
- new_state: float32 [512, 32, 128, 128], P(None, 'head', 'row')
The draws below stay inside these ranges and needn't reach their ends.
All inputs are finite; a program needn't handle non-finite values.
Results may differ from the reference program's by a relative error of at most 0.005.
Values sent between devices are 32-bit elements; how exact they have to be, the bound alone decides.
No kernel may reach another device: no remote copies, remote signals or barrier semaphores. Data moves between devices by JAX's collectives and lax.ppermute only.
A program may use at most 128 MiB of HBM per device.

```python
import jax
import jax.numpy as jnp
from jax import lax

D = 2048
H = 32
HK = 16
K = 128
V = 128
SEQS = 512


def block_levels(rng, extent, shards, least, top_value):
    loudness = 1.0
    for dim, parts in shards:
        draws = jax.random.uniform(jax.random.fold_in(jax.random.fold_in(rng, 6), dim), (parts,), jnp.float32, least / len(shards), top_value / len(shards))
        loudness = loudness * jnp.repeat(jnp.exp(draws), extent[dim] // parts).reshape((-1,) + (1,) * (len(extent) - 1 - dim))
    return loudness


def noise(key, extent, width, reach, split=(), held_as=jnp.bfloat16):
    result = width * jax.random.normal(key, extent, jnp.float32)
    if split:
        result = result * block_levels(key, extent, split, -0.22, 0.18)
    return jnp.clip(result, -reach, reach).astype(held_as)


def setup_inputs(seed: int = 0) -> dict:
    arg_keys = jax.random.split(jax.random.key(seed), 13)
    hidden_in = noise(arg_keys[0], (SEQS, D), 1.0, 6.0)
    w_query = noise(arg_keys[1], (D, HK, K), D ** -0.5, 0.125, ((1, 8), (2, 16)))
    w_key = noise(arg_keys[2], (D, HK, K), D ** -0.5, 0.125, ((1, 8), (2, 16)))
    w_value = noise(arg_keys[3], (D, H, V), D ** -0.5, 0.125, ((1, 8),))
    w_zgate = noise(arg_keys[4], (D, H, V), D ** -0.5, 0.125, ((1, 8),))
    w_decay = noise(arg_keys[5], (D, H), D ** -0.5, 0.125, ((1, 8),))
    w_beta = noise(arg_keys[6], (D, H), D ** -0.5, 0.125, ((1, 8),))
    decay_log = jnp.clip(jax.random.uniform(arg_keys[7], (H,), jnp.float32, -1.5, 1.5) * block_levels(arg_keys[7], (H,), ((0, 8),), -0.4, 0.0), -1.5, 1.5)
    dt_bias = jnp.clip(jax.random.uniform(arg_keys[8], (H,), jnp.float32, -2.0, 2.0) * block_levels(arg_keys[8], (H,), ((0, 8),), -0.4, 0.0), -2.0, 2.0)
    norm_gain = jnp.clip(1.0 + 0.18 * jax.random.normal(arg_keys[9], (V,), jnp.float32), 0.1, 1.9)
    w_out = noise(arg_keys[10], (H, V, D), (H * V) ** -0.5, 0.09375, ((0, 8),))
    state = noise(arg_keys[11], (SEQS, H, K, V), 1.0, 6.0, ((1, 8), (2, 16)), jnp.float32)
    return {"hidden_in": hidden_in, "w_query": w_query, "w_key": w_key, "w_value": w_value, "w_zgate": w_zgate, "w_decay": w_decay, "w_beta": w_beta, "decay_log": decay_log, "dt_bias": dt_bias, "norm_gain": norm_gain, "w_out": w_out, "state": state}


def reference(hidden_in, w_query, w_key, w_value, w_zgate, w_decay, w_beta, decay_log, dt_bias, norm_gain, w_out, state):
    xf = hidden_in.astype(jnp.float32)
    query = jnp.einsum('bd,dhk->bhk', xf, w_query.astype(jnp.float32))
    keys = jnp.einsum('bd,dhk->bhk', xf, w_key.astype(jnp.float32))
    values = jnp.einsum('bd,dhv->bhv', xf, w_value.astype(jnp.float32))
    zgate = jnp.einsum('bd,dhv->bhv', xf, w_zgate.astype(jnp.float32))
    decay_in = jnp.dot(hidden_in, w_decay, preferred_element_type=jnp.float32) + dt_bias
    decay = jnp.exp(-jnp.exp(decay_log) * jax.nn.softplus(decay_in))
    beta = jax.nn.sigmoid(jnp.dot(hidden_in, w_beta, preferred_element_type=jnp.float32))
    group = state.shape[1] // keys.shape[1]
    query_unit = query * lax.rsqrt(1.0 + lax.optimization_barrier(jnp.sum(query * query, axis=-1, keepdims=True)))
    key_unit = keys * lax.rsqrt(1.0 + lax.optimization_barrier(jnp.sum(keys * keys, axis=-1, keepdims=True)))
    query_wide = jnp.repeat(query_unit, group, axis=1)
    key_wide = jnp.repeat(key_unit, group, axis=1)
    readk = jnp.einsum('bhkv,bhk->bhv', state, key_wide, precision=lax.Precision.HIGHEST)
    delta = beta[..., None] * (values - decay[..., None] * readk)
    new_state = decay[..., None, None] * state + key_wide[..., None] * delta[:, :, None, :]
    readq = jnp.einsum('bhkv,bhk->bhv', new_state, query_wide, precision=lax.Precision.HIGHEST)
    meansq = lax.optimization_barrier(jnp.mean(readq * readq, axis=-1, keepdims=True))
    normed = (readq * lax.rsqrt(meansq + 0.5) * norm_gain * jax.nn.silu(zgate)).astype(jnp.bfloat16)
    layer_out = jnp.einsum('bhv,hvd->bd', normed.astype(jnp.float32), w_out.astype(jnp.float32))
    return (layer_out.astype(jnp.bfloat16), new_state)
```

```python
import jax
import jax.numpy as jnp
from jax import lax
from jax.experimental import pallas as pl
from jax.experimental.pallas import tpu as pltpu
from jax.sharding import PartitionSpec as P

LANES = 128
SUB = 8


def spread(column):
    return jnp.broadcast_to(column, (SUB, LANES))


def rows_summed(tiles, row):
    step = 1
    while len(tiles) > 1:
        keep = (row & step) != 0
        merged = []
        for low, high in zip(tiles[0::2], tiles[1::2]):
            merged.append(jnp.where(keep, high, low) + pltpu.roll(jnp.where(keep, low, high), step, 0))
        tiles = merged
        step *= 2
    return tiles[0]


def own_lanes(ref, part, rows):
    per_tile = LANES // rows
    tile = ref[:, pl.ds(pl.multiple_of(part // per_tile * LANES, LANES), LANES)]
    shift = (LANES - part % per_tile * rows) % LANES
    return pltpu.roll(tile, shift, 1)


def read_kernel(hidden, w_query, w_key, w_decay, decay_log, dt_bias, state, sent, keys_out, decay_out, weights, vectors, sums):
    part = pl.program_id(0)
    key_rows = w_query.shape[0]
    heads = w_decay.shape[0]
    seqs = hidden.shape[0]
    rows = state.shape[0]
    key_heads = key_rows // SUB
    group = heads // key_heads

    @pl.when(part == 0)
    def _():
        weights[...] = jnp.zeros(weights.shape, weights.dtype)
        weights[0:key_rows] = w_query[...]
        weights[key_rows : 2 * key_rows] = w_key[...]
        weights[2 * key_rows : 2 * key_rows + heads] = w_decay[...]
        projected = lax.dot_general(weights[...], hidden[...], (((1,), (1,)), ((), ())), preferred_element_type=jnp.float32)
        query = projected[0:key_rows]
        keys = projected[key_rows : 2 * key_rows]
        vectors[...] = projected[0 : 2 * key_rows]
        keys_out[...] = keys
        pre = projected[2 * key_rows : 2 * key_rows + heads] + dt_bias[...]
        soft = jnp.maximum(pre, 0.0) + jnp.log1p(jnp.exp(-jnp.abs(pre)))
        decay = jnp.exp(-jnp.exp(decay_log[...]) * soft)
        for h in range(heads):
            decay_out[h * SUB : (h + 1) * SUB] = jnp.broadcast_to(decay[h : h + 1], (SUB, seqs))
        sums[...] = jnp.zeros(sums.shape, sums.dtype)
        for n, product in enumerate((query * query, keys * keys, query * keys)):
            for g in range(key_heads):
                sums[n * key_heads + g : n * key_heads + g + 1] = jnp.sum(product[g * SUB : (g + 1) * SUB], axis=0, keepdims=True)

    row = lax.broadcasted_iota(jnp.int32, (SUB, LANES), 0)
    mine = own_lanes(vectors, part, rows)
    for first in range(0, rows, SUB):
        for g in range(key_heads):
            by_key = [[] for _ in range(group)]
            by_query = [[] for _ in range(group)]
            for b in range(first, first + SUB):
                q = spread(mine[g * SUB : (g + 1) * SUB, b : b + 1])
                k = spread(mine[key_rows + g * SUB : key_rows + (g + 1) * SUB, b : b + 1])
                for j in range(group):
                    tile = state[b, g * group + j]
                    by_key[j].append(tile * k)
                    by_query[j].append(tile * q)
            for j in range(group):
                h = g * group + j
                sent[0, h * rows + first : h * rows + first + SUB] = rows_summed(by_key[j], row)
                at = (heads + h) * rows + first
                sent[0, at : at + SUB] = rows_summed(by_query[j], row)
    sent[0, 2 * heads * rows : 2 * heads * rows + SUB] = own_lanes(sums, part, rows)


def owner_kernel(arrived, values, zgate, decay, beta, norm_gain, delta_out, normed_out):
    rows, heads = decay.shape
    key_heads = 2
    group = heads // key_heads
    total = arrived[0]
    for n in range(1, arrived.shape[0]):
        total = total + arrived[n]
    sums = jnp.transpose(total[2 * heads * rows :])[0:rows]
    query_scale = lax.rsqrt(1.0 + sums[:, 0:key_heads])
    key_scale = lax.rsqrt(1.0 + sums[:, key_heads : 2 * key_heads])
    unit_dot = sums[:, 2 * key_heads : 3 * key_heads] * query_scale * key_scale
    for h in range(heads):
        g = h // group
        lanes = slice(h * LANES, (h + 1) * LANES)
        d = decay[:, h : h + 1]
        ks = key_scale[:, g : g + 1]
        readk = total[h * rows : (h + 1) * rows] * ks
        delta = beta[:, h : h + 1] * (values[:, lanes] - d * readk)
        raw_q = total[(heads + h) * rows : (heads + h + 1) * rows]
        readq = d * (raw_q * query_scale[:, g : g + 1]) + unit_dot[:, g : g + 1] * delta
        meansq = jnp.mean(readq * readq, axis=1, keepdims=True)
        z = zgate[:, lanes]
        normed = readq * lax.rsqrt(meansq + 0.5) * norm_gain[...] * (z / (1.0 + jnp.exp(-z)))
        normed_out[:, lanes] = normed.astype(jnp.bfloat16)
        scaled = delta * ks
        for n in range(delta_out.shape[0]):
            delta_out[n, h * rows : (h + 1) * rows] = scaled


def update_kernel(keys, decay, delta, state, new_state):
    part = pl.program_id(0)
    rows, heads = state.shape[0:2]
    key_heads = keys.shape[0] // SUB
    group = heads // key_heads
    my_keys = own_lanes(keys, part, rows)
    my_decay = own_lanes(decay, part, rows)
    for b in range(rows):
        for g in range(key_heads):
            k = spread(my_keys[g * SUB : (g + 1) * SUB, b : b + 1])
            for h in range(g * group, (g + 1) * group):
                d = spread(my_decay[h * SUB : (h + 1) * SUB, b : b + 1])
                row = jnp.broadcast_to(delta[0, h * rows + b : h * rows + b + 1], (SUB, LANES))
                new_state[b, h] = d * state[b, h] + k * row


def local(
    hidden_in,
    w_query,
    w_key,
    w_value,
    w_zgate,
    w_decay,
    w_beta,
    decay_log,
    dt_bias,
    norm_gain,
    w_out,
    state,
):
    parts = lax.axis_size("row")
    seqs, width = hidden_in.shape
    rows = seqs // parts
    heads = state.shape[1]
    key_rows = w_query.shape[1] * w_query.shape[2]
    per_part = 2 * heads * rows + SUB
    f32 = jnp.float32

    def whole(*shape):
        return pl.BlockSpec(shape, lambda n: (0,) * len(shape))

    state_block = pl.BlockSpec((rows, heads, SUB, LANES), lambda n: (n, 0, 0, 0))
    limit = pltpu.CompilerParams(vmem_limit_bytes=24 * 1024 * 1024)
    sent, keys, decay_wide = pl.pallas_call(
        read_kernel,
        grid=(parts,),
        in_specs=[
            whole(seqs, width),
            whole(key_rows, width),
            whole(key_rows, width),
            whole(heads, width),
            whole(heads, 1),
            whole(heads, 1),
            state_block,
        ],
        out_specs=[
            pl.BlockSpec((1, per_part, LANES), lambda n: (n, 0, 0)),
            whole(key_rows, seqs),
            whole(heads * SUB, seqs),
        ],
        out_shape=[
            jax.ShapeDtypeStruct((parts, per_part, LANES), f32),
            jax.ShapeDtypeStruct((key_rows, seqs), f32),
            jax.ShapeDtypeStruct((heads * SUB, seqs), f32),
        ],
        scratch_shapes=[
            pltpu.VMEM((2 * key_rows + 16, width), jnp.bfloat16),
            pltpu.VMEM((2 * key_rows, seqs), f32),
            pltpu.VMEM((SUB, seqs), f32),
        ],
        compiler_params=limit,
        name="read_state",
    )(
        hidden_in,
        jnp.transpose(w_query, (1, 2, 0)).reshape(key_rows, width),
        jnp.transpose(w_key, (1, 2, 0)).reshape(key_rows, width),
        jnp.transpose(w_decay),
        decay_log[:, None],
        dt_bias[:, None],
        state,
    )
    arrived = lax.all_to_all(sent, "row", 0, 0, tiled=True)

    own_hidden = lax.dynamic_slice_in_dim(hidden_in, lax.axis_index("row") * rows, rows, 0)
    values = jnp.einsum("bd,dhv->bhv", own_hidden, w_value, preferred_element_type=f32).reshape(rows, heads * LANES)
    zgate = jnp.einsum("bd,dhv->bhv", own_hidden, w_zgate, preferred_element_type=f32).reshape(rows, heads * LANES)
    decay_in = jnp.dot(own_hidden, w_decay, preferred_element_type=f32) + dt_bias
    decay = jnp.exp(-jnp.exp(decay_log) * jax.nn.softplus(decay_in))
    beta = jax.nn.sigmoid(jnp.dot(own_hidden, w_beta, preferred_element_type=f32))

    delta_own, normed = pl.pallas_call(
        owner_kernel,
        out_shape=[
            jax.ShapeDtypeStruct((parts, heads * rows, LANES), f32),
            jax.ShapeDtypeStruct((rows, heads * LANES), jnp.bfloat16),
        ],
        compiler_params=limit,
        name="owner_rows",
    )(arrived, values, zgate, decay, beta, norm_gain[None])
    delta = lax.all_to_all(delta_own, "row", 0, 0, tiled=True)

    partial_out = jnp.dot(normed, w_out.reshape(heads * LANES, -1), preferred_element_type=f32)
    tall = lax.axis_size("head")
    pieces = jnp.moveaxis(partial_out.reshape(rows, tall, -1), 1, 0)
    pieces = lax.all_to_all(pieces, "head", 0, 0, tiled=True)
    layer_out = jnp.sum(pieces, axis=0).astype(jnp.bfloat16)

    new_state = pl.pallas_call(
        update_kernel,
        grid=(parts,),
        in_specs=[
            whole(key_rows, seqs),
            whole(heads * SUB, seqs),
            pl.BlockSpec((1, heads * rows, LANES), lambda n: (n, 0, 0)),
            state_block,
        ],
        out_specs=state_block,
        out_shape=jax.ShapeDtypeStruct(state.shape, f32),
        compiler_params=limit,
        name="update_state",
    )(keys, decay_wide, delta, state)
    return (layer_out, new_state)


def solution(mesh):
    in_specs = (
        P(),
        P(None, "head", "row"),
        P(None, "head", "row"),
        P(None, "head", None),
        P(None, "head", None),
        P(None, "head"),
        P(None, "head"),
        P("head"),
        P("head"),
        P(),
        P("head", None, None),
        P(None, "head", "row", None),
    )
    out_specs = (P("row", "head"), P(None, "head", "row", None))
    return jax.shard_map(local, mesh=mesh, in_specs=in_specs, out_specs=out_specs, check_vma=False)
```

```python
import jax
import jax.numpy as jnp
from jax import lax
from jax.experimental import pallas as pl
from jax.experimental.pallas import tpu as pltpu
from jax.sharding import PartitionSpec as P


LANES = 128
SUB = 8


def high_low(value):
    high = value.astype(jnp.bfloat16)
    return high, (value - high.astype(jnp.float32)).astype(jnp.bfloat16)


def dot(left, right):
    return jnp.dot(left, right, preferred_element_type=jnp.float32)


def own_lanes(ref, part, rows):
    per_tile = LANES // rows
    tile = ref[:, pl.ds(pl.multiple_of(part // per_tile * LANES, LANES), LANES)]
    shift = (LANES - part % per_tile * rows) % LANES
    return pltpu.roll(tile, shift, 1)


def read_kernel(
    hidden_hbm,
    w_query_hbm,
    w_key_hbm,
    w_decay_hbm,
    decay_log_hbm,
    dt_bias_hbm,
    state_hbm,
    sent_hbm,
    keys_out,
    decay_out,
    hidden,
    weights,
    w_decay,
    decay_log,
    dt_bias,
    state,
    sent,
    picks_high,
    picks_low,
    sums,
    in_sems,
    state_sems,
    sent_sems,
):
    parts, rows, heads = state.shape[0:3]
    key_rows = w_query_hbm.shape[0]
    key_heads = key_rows // SUB
    group = heads // key_heads
    span = rows * SUB
    pad = weights.dtype.itemsize * SUB

    inputs = [
        pltpu.make_async_copy(hidden_hbm, hidden, in_sems.at[0]),
        pltpu.make_async_copy(w_query_hbm, weights.at[pad : pad + key_rows], in_sems.at[1]),
        pltpu.make_async_copy(w_key_hbm, weights.at[pad + key_rows : pad + 2 * key_rows], in_sems.at[2]),
        pltpu.make_async_copy(w_decay_hbm, w_decay, in_sems.at[3]),
        pltpu.make_async_copy(decay_log_hbm, decay_log, in_sems.at[4]),
        pltpu.make_async_copy(dt_bias_hbm, dt_bias, in_sems.at[5]),
    ]
    for copy in inputs:
        copy.start()

    def state_copy(n):
        return pltpu.make_async_copy(state_hbm.at[pl.ds(n * rows, rows)], state.at[n], state_sems.at[n])

    def sent_copy(n):
        return pltpu.make_async_copy(sent.at[n], sent_hbm.at[n], sent_sems.at[n])

    for n in range(parts):
        state_copy(n).start()
    width = weights.shape[1]
    weights[0:pad] = jnp.zeros((pad, width), weights.dtype)
    weights[pad + 2 * key_rows :] = jnp.zeros((LANES - pad - 2 * key_rows, width), weights.dtype)
    for copy in inputs:
        copy.wait()
    weights[0:heads] = w_decay[...]
    projected = lax.dot_general(hidden[...], weights[...], (((1,), (1,)), ((), ())), preferred_element_type=jnp.float32)
    high, low = high_low(projected)
    source = lax.broadcasted_iota(jnp.int32, (LANES, span), 0)
    entry = lax.broadcasted_iota(jnp.int32, (LANES, span), 1) % SUB
    own = lax.broadcasted_iota(jnp.int32, (rows, span), 1) // SUB == lax.broadcasted_iota(jnp.int32, (rows, span), 0)
    for kind in range(2):
        for g in range(key_heads):
            pick = (source == pad + kind * key_rows + g * SUB + entry).astype(jnp.bfloat16)
            for half, picks in ((high, picks_high), (low, picks_low)):
                wide = dot(half, pick).reshape(parts, rows, span)
                picks[:, g, kind * rows : (kind + 1) * rows] = jnp.where(own[None], wide, 0.0).astype(jnp.bfloat16)

    pre = projected[:, 0:heads] + dt_bias[...]
    soft = jnp.maximum(pre, 0.0) + jnp.log1p(jnp.exp(-jnp.abs(pre)))
    decay_out[...] = jnp.exp(-jnp.exp(decay_log[...]) * soft)

    turned = jnp.transpose(projected)
    query = turned[pad : pad + key_rows]
    keys = turned[pad + key_rows : pad + 2 * key_rows]
    keys_out[...] = keys
    sums[...] = jnp.zeros(sums.shape, sums.dtype)
    for n, product in enumerate((query * query, keys * keys, query * keys)):
        for g in range(key_heads):
            sums[n * key_heads + g : n * key_heads + g + 1] = jnp.sum(product[g * SUB : (g + 1) * SUB], axis=0, keepdims=True)

    @pl.loop(0, parts)
    def _(part):
        state_copy(part).wait()
        for g in range(key_heads):
            tiles = [state[part, :, g * group + j].reshape(span, LANES) for j in range(group)]
            state_high, state_low = high_low(jnp.concatenate(tiles, axis=1))
            pick_high = picks_high[part, g]
            both = dot(jnp.concatenate([pick_high, picks_low[part, g]], axis=0), state_high)
            read = both[0 : 2 * rows] + both[2 * rows :] + dot(pick_high, state_low)
            for j in range(group):
                at = (g * group + j) * rows
                lanes = slice(j * LANES, (j + 1) * LANES)
                sent[part, at : at + rows] = read[rows:, lanes]
                at += heads * rows
                sent[part, at : at + rows] = read[0:rows, lanes]
        sent[part, 2 * heads * rows : 2 * heads * rows + SUB] = own_lanes(sums, part, rows)
        sent_copy(part).start()

    @pl.loop(0, parts)
    def _(part):
        sent_copy(part).wait()


def owner_kernel(arrived, values, zgate, decay, beta, norm_gain, delta_out, normed_out):
    rows, heads = decay.shape
    key_heads = 2
    group = heads // key_heads
    total = arrived[0]
    for n in range(1, arrived.shape[0]):
        total = total + arrived[n]
    sums = jnp.transpose(total[2 * heads * rows :])[0:rows]
    query_scale = lax.rsqrt(1.0 + sums[:, 0:key_heads])
    key_scale = lax.rsqrt(1.0 + sums[:, key_heads : 2 * key_heads])
    unit_dot = sums[:, 2 * key_heads : 3 * key_heads] * query_scale * key_scale
    for h in range(heads):
        g = h // group
        lanes = slice(h * LANES, (h + 1) * LANES)
        d = decay[:, h : h + 1]
        ks = key_scale[:, g : g + 1]
        readk = total[h * rows : (h + 1) * rows] * ks
        delta = beta[:, h : h + 1] * (values[:, lanes] - d * readk)
        raw_q = total[(heads + h) * rows : (heads + h + 1) * rows]
        readq = d * (raw_q * query_scale[:, g : g + 1]) + unit_dot[:, g : g + 1] * delta
        meansq = jnp.mean(readq * readq, axis=1, keepdims=True)
        z = zgate[:, lanes]
        normed = readq * lax.rsqrt(meansq + 0.5) * norm_gain[...] * (z / (1.0 + jnp.exp(-z)))
        normed_out[:, lanes] = normed.astype(jnp.bfloat16)
        scaled = delta * ks
        for n in range(delta_out.shape[0]):
            delta_out[n, h * rows : (h + 1) * rows] = scaled


def update_kernel(keys, decay, delta, state_hbm, new_state, state, ready, in_sems, out_sems):
    parts, rows, heads = state.shape[0:3]
    key_heads = keys.shape[0] // SUB
    group = heads // key_heads
    span = rows * SUB

    def read(n):
        return pltpu.make_async_copy(state_hbm.at[pl.ds(n * rows, rows)], state.at[n], in_sems.at[n])

    def write(n):
        return pltpu.make_async_copy(ready.at[n], new_state.at[pl.ds(n * rows, rows)], out_sems.at[n])

    for n in range(parts):
        read(n).start()
    lane = lax.broadcasted_iota(jnp.int32, (SUB, LANES), 1)
    slot = lax.broadcasted_iota(jnp.int32, (span, LANES), 1)
    own = (slot % rows == lax.broadcasted_iota(jnp.int32, (span, LANES), 0) // SUB) & (slot < 3 * rows)
    ones = own.astype(jnp.bfloat16)
    none = jnp.zeros((LANES - 3 * rows, group * LANES), jnp.bfloat16)

    @pl.loop(0, parts)
    def _(part):
        my_keys = own_lanes(keys, part, rows)
        my_decay = decay[pl.ds(pl.multiple_of(part * rows, rows), rows)]
        read(part).wait()
        for g in range(key_heads):
            key = my_keys[g * SUB : (g + 1) * SUB]
            high = key.astype(jnp.bfloat16).astype(jnp.float32)
            low = key - high
            packed = jnp.where(lane < rows, high, jnp.where(lane < 2 * rows, pltpu.roll(low, rows, 1), pltpu.roll(high, 2 * rows, 1)))
            spread = jnp.broadcast_to(packed[None], (rows, SUB, LANES)).reshape(span, LANES)
            left = jnp.where(own, spread, 0.0).astype(jnp.bfloat16)
            own_heads = range(g * group, (g + 1) * group)
            d_high, d_low = high_low(jnp.concatenate([delta[part, h * rows : (h + 1) * rows] for h in own_heads], axis=1))
            outer = dot(left, jnp.concatenate([d_high, d_high, d_low, none], axis=0))
            wide = jnp.concatenate([jnp.broadcast_to(my_decay[:, h : h + 1], (rows, LANES)) for h in own_heads], axis=1)
            w_high = wide.astype(jnp.bfloat16)
            rest = wide - w_high.astype(jnp.float32)
            w_mid, w_low = high_low(rest)
            factor = dot(ones, jnp.concatenate([w_high, w_mid, w_low, none], axis=0))
            for j, h in enumerate(own_heads):
                lanes = slice(j * LANES, (j + 1) * LANES)
                f = factor[:, lanes].reshape(rows, SUB, LANES)
                ready[part, :, h] = f * state[part, :, h] + outer[:, lanes].reshape(rows, SUB, LANES)
        write(part).start()

    @pl.loop(0, parts)
    def _(part):
        write(part).wait()


def project_kernel(core, normed, w_out_hbm, give, keep, w_out, sem):
    copy = pltpu.make_async_copy(w_out_hbm, w_out, sem)
    copy.start()
    copy.wait()
    total = dot(normed[...], w_out[...])
    size = give.shape[2]
    first = core[0] == 0
    for y in range(give.shape[0]):
        even = total[:, 2 * y * size : (2 * y + 1) * size]
        odd = total[:, (2 * y + 1) * size : (2 * y + 2) * size]
        keep[y] = jnp.where(first, even, odd)
        give[y] = jnp.where(first, odd, even)


def chip_kernel(y, keep, got, own, *away):
    size = keep.shape[0]
    own[...] = keep[y[0]] + got[y[0]]
    for n, out in enumerate(away):
        at = (y[0] + n + 1) % size
        out[...] = keep[at] + got[at]


def head_exchange(normed, w_out, y_size):
    rows = normed.shape[0]
    heads = 2 * y_size
    size = w_out.shape[1] // heads
    head = lax.axis_index("head")
    in_smem = pl.BlockSpec(memory_space=pltpu.SMEM)
    in_vmem = pl.BlockSpec(memory_space=pltpu.VMEM)
    limit = pltpu.CompilerParams(vmem_limit_bytes=8 * 1024 * 1024)
    piece = jax.ShapeDtypeStruct((y_size, rows, size), jnp.float32)
    give, keep = pl.pallas_call(
        project_kernel,
        in_specs=[in_smem, in_vmem, pl.BlockSpec(memory_space=pl.ANY)],
        out_specs=[in_vmem, in_vmem],
        out_shape=[piece, piece],
        scratch_shapes=[pltpu.VMEM(w_out.shape, w_out.dtype), pltpu.SemaphoreType.DMA],
        compiler_params=limit,
        name="project_out",
    )((head % 2)[None], normed, pltpu.with_memory_space_constraint(w_out, pltpu.HBM))
    got = lax.ppermute(give, "head", [(h, h ^ 1) for h in range(heads)])
    total, *away = pl.pallas_call(
        chip_kernel,
        in_specs=[in_smem, in_vmem, in_vmem],
        out_specs=[in_vmem] * y_size,
        out_shape=[jax.ShapeDtypeStruct((rows, size), jnp.float32)] * y_size,
        compiler_params=limit,
        name="chip_sum",
    )((head // 2)[None], keep, got)
    for s, part in enumerate(away, 1):
        total = total + lax.ppermute(part, "head", [(h, (h + 2 * s) % heads) for h in range(heads)])
    return total


def decode(
    hidden_in,
    w_query,
    w_key,
    w_value,
    w_zgate,
    w_decay,
    w_beta,
    decay_log,
    dt_bias,
    norm_gain,
    w_out,
    state,
):
    parts = lax.axis_size("row")
    seqs, width = hidden_in.shape
    rows = seqs // parts
    heads = state.shape[1]
    key_rows = w_query.shape[1] * w_query.shape[2]
    per_part = 2 * heads * rows + SUB
    f32 = jnp.float32

    def in_hbm(value):
        return pltpu.with_memory_space_constraint(value, pltpu.HBM)

    any_space = pl.BlockSpec(memory_space=pl.ANY)
    in_vmem = pl.BlockSpec(memory_space=pltpu.VMEM)
    limit = pltpu.CompilerParams(vmem_limit_bytes=20 * 1024 * 1024)
    sent, keys, decay_all = pl.pallas_call(
        read_kernel,
        in_specs=[any_space] * 7,
        out_specs=[any_space, in_vmem, in_vmem],
        out_shape=[
            pltpu.HBM((parts, per_part, LANES), f32),
            pltpu.VMEM((key_rows, seqs), f32),
            pltpu.VMEM((seqs, heads), f32),
        ],
        scratch_shapes=[
            pltpu.VMEM((seqs, width), jnp.bfloat16),
            pltpu.VMEM((LANES, width), jnp.bfloat16),
            pltpu.VMEM((heads, width), jnp.bfloat16),
            pltpu.VMEM((1, heads), f32),
            pltpu.VMEM((1, heads), f32),
            pltpu.VMEM((parts, rows, heads, SUB, LANES), f32),
            pltpu.VMEM((parts, per_part, LANES), f32),
            pltpu.VMEM((parts, key_rows // SUB, 2 * rows, rows * SUB), jnp.bfloat16),
            pltpu.VMEM((parts, key_rows // SUB, 2 * rows, rows * SUB), jnp.bfloat16),
            pltpu.VMEM((SUB, seqs), f32),
            pltpu.SemaphoreType.DMA((6,)),
            pltpu.SemaphoreType.DMA((parts,)),
            pltpu.SemaphoreType.DMA((parts,)),
        ],
        compiler_params=limit,
        name="read_state",
    )(
        in_hbm(hidden_in),
        in_hbm(jnp.transpose(w_query, (1, 2, 0)).reshape(key_rows, width)),
        in_hbm(jnp.transpose(w_key, (1, 2, 0)).reshape(key_rows, width)),
        in_hbm(jnp.transpose(w_decay)),
        in_hbm(decay_log[None]),
        in_hbm(dt_bias[None]),
        in_hbm(state),
    )
    arrived = lax.all_to_all(sent, "row", 0, 0, tiled=True)

    own_hidden = lax.dynamic_slice_in_dim(hidden_in, lax.axis_index("row") * rows, rows, 0)
    values = jnp.einsum("bd,dhv->bhv", own_hidden, w_value, preferred_element_type=f32).reshape(rows, heads * LANES)
    zgate = jnp.einsum("bd,dhv->bhv", own_hidden, w_zgate, preferred_element_type=f32).reshape(rows, heads * LANES)
    decay_in = jnp.dot(own_hidden, w_decay, preferred_element_type=f32) + dt_bias
    decay = jnp.exp(-jnp.exp(decay_log) * jax.nn.softplus(decay_in))
    beta = jax.nn.sigmoid(jnp.dot(own_hidden, w_beta, preferred_element_type=f32))

    delta_own, normed = pl.pallas_call(
        owner_kernel,
        out_shape=[
            jax.ShapeDtypeStruct((parts, heads * rows, LANES), f32),
            jax.ShapeDtypeStruct((rows, heads * LANES), jnp.bfloat16),
        ],
        compiler_params=limit,
        name="owner_rows",
    )(arrived, values, zgate, decay, beta, norm_gain[None])
    delta = lax.all_to_all(delta_own, "row", 0, 0, tiled=True)

    layer_out = head_exchange(normed, w_out.reshape(heads * LANES, -1), lax.axis_size("head") // 2).astype(jnp.bfloat16)

    new_state = pl.pallas_call(
        update_kernel,
        in_specs=[in_vmem, in_vmem, in_vmem, any_space],
        out_specs=any_space,
        out_shape=pltpu.HBM(state.shape, f32),
        scratch_shapes=[
            pltpu.VMEM((parts, rows, heads, SUB, LANES), f32),
            pltpu.VMEM((parts, rows, heads, SUB, LANES), f32),
            pltpu.SemaphoreType.DMA((parts,)),
            pltpu.SemaphoreType.DMA((parts,)),
        ],
        compiler_params=pltpu.CompilerParams(vmem_limit_bytes=24 * 1024 * 1024),
        name="update_state",
    )(keys, decay_all, delta, in_hbm(state))
    return (layer_out, new_state)


def solution(mesh):
    in_specs = (
        P(),
        P(None, "head", "row"),
        P(None, "head", "row"),
        P(None, "head", None),
        P(None, "head", None),
        P(None, "head"),
        P(None, "head"),
        P("head"),
        P("head"),
        P(),
        P("head", None, None),
        P(None, "head", "row", None),
    )
    out_specs = (P("row", "head"), P(None, "head", "row", None))
    return jax.shard_map(decode, mesh=mesh, in_specs=in_specs, out_specs=out_specs, check_vma=False)
```

```python
import jax
import jax.numpy as jnp
from jax import lax
from jax.experimental import pallas as pl
from jax.experimental.pallas import tpu as pltpu
from jax.sharding import PartitionSpec as P


LANES = 128
SUB = 8


def high_low(value):
    high = value.astype(jnp.bfloat16)
    return high, (value - high.astype(jnp.float32)).astype(jnp.bfloat16)


def dot(left, right):
    return jnp.dot(left, right, preferred_element_type=jnp.float32)


def read_kernel(
    hidden_hbm,
    w_query_hbm,
    w_key_hbm,
    w_decay_hbm,
    decay_log_hbm,
    dt_bias_hbm,
    state_hbm,
    sent_hbm,
    keys_hbm,
    decay_hbm,
    hidden,
    weights,
    w_decay,
    decay_log,
    dt_bias,
    state,
    sent,
    picks,
    sums,
    keys_all,
    decay_all,
    in_sems,
    hidden_sems,
    state_sems,
    sent_sems,
    out_sems,
):
    parts, rows, heads = state.shape[0:3]
    chunks = hidden.shape[0]
    per_chunk = parts // chunks
    key_rows = w_query_hbm.shape[0]
    key_heads = key_rows // SUB
    group = heads // key_heads
    span = rows * SUB
    pad = weights.dtype.itemsize * SUB

    inputs = [
        pltpu.make_async_copy(w_query_hbm, weights.at[pad : pad + key_rows], in_sems.at[0]),
        pltpu.make_async_copy(w_key_hbm, weights.at[pad + key_rows : pad + 2 * key_rows], in_sems.at[1]),
        pltpu.make_async_copy(w_decay_hbm, w_decay, in_sems.at[2]),
        pltpu.make_async_copy(decay_log_hbm, decay_log, in_sems.at[3]),
        pltpu.make_async_copy(dt_bias_hbm, dt_bias, in_sems.at[4]),
    ]
    for copy in inputs:
        copy.start()

    def hidden_copy(n):
        return pltpu.make_async_copy(hidden_hbm.at[pl.ds(n * LANES, LANES)], hidden.at[n], hidden_sems.at[n])

    def state_copy(n):
        return pltpu.make_async_copy(state_hbm.at[pl.ds(n * rows, rows)], state.at[n], state_sems.at[n])

    def sent_copy(n):
        return pltpu.make_async_copy(sent.at[n], sent_hbm.at[n], sent_sems.at[n])

    ahead = 8
    for n in range(chunks):
        hidden_copy(n).start()
    width = weights.shape[1]
    weights[0:pad] = jnp.zeros((pad, width), weights.dtype)
    weights[pad + 2 * key_rows :] = jnp.zeros((LANES - pad - 2 * key_rows, width), weights.dtype)
    sums[...] = jnp.zeros(sums.shape, sums.dtype)
    source = lax.broadcasted_iota(jnp.int32, (LANES, span), 0)
    entry = lax.broadcasted_iota(jnp.int32, (LANES, span), 1) % SUB
    own = lax.broadcasted_iota(jnp.int32, (rows, span), 1) // SUB == lax.broadcasted_iota(jnp.int32, (rows, span), 0)
    for n in range(2 * key_heads):
        picks[n] = (source == pad + n * SUB + entry).astype(jnp.bfloat16)
    for copy in inputs:
        copy.wait()
    weights[0:heads] = w_decay[...]

    @pl.loop(0, chunks)
    def _(chunk):
        hidden_copy(chunk).wait()

        @pl.when(chunk == 0)
        def _():
            for n in range(ahead):
                state_copy(n).start()

        projected = lax.dot_general(hidden[chunk], weights[...], (((1,), (1,)), ((), ())), preferred_element_type=jnp.float32)
        halves = jnp.concatenate(high_low(projected), axis=0)
        left = []
        for n in range(2 * key_heads):
            wide = dot(halves, picks[n]).reshape(2 * per_chunk, rows, span)
            left.append(jnp.where(own[None], wide, 0.0).astype(jnp.bfloat16))

        at = pl.multiple_of(chunk * LANES, LANES)
        pre = projected[:, 0:heads] + dt_bias[...]
        soft = jnp.maximum(pre, 0.0) + jnp.log1p(jnp.exp(-jnp.abs(pre)))
        decay_all[pl.ds(at, LANES)] = jnp.exp(-jnp.exp(decay_log[...]) * soft)
        turned = jnp.transpose(projected)
        query = turned[pad : pad + key_rows]
        keys = turned[pad + key_rows : pad + 2 * key_rows]
        keys_all[:, pl.ds(at, LANES)] = keys
        for n, product in enumerate((query * query, keys * keys, query * keys)):
            for g in range(key_heads):
                sums[n * key_heads + g : n * key_heads + g + 1] = jnp.sum(product[g * SUB : (g + 1) * SUB], axis=0, keepdims=True)

        for p in range(per_chunk):
            part = chunk * per_chunk + p
            state_copy(part).wait()

            @pl.when(part + ahead < parts)
            def _():
                state_copy(part + ahead).start()

            for g in range(key_heads):
                tiles = [state[part, :, g * group + j].reshape(span, LANES) for j in range(group)]
                state_high, state_low = high_low(jnp.concatenate(tiles, axis=1))
                q_left, k_left = left[g], left[key_heads + g]
                high = jnp.concatenate([q_left[p], k_left[p]], axis=0)
                both = dot(jnp.concatenate([high, q_left[per_chunk + p], k_left[per_chunk + p]], axis=0), state_high)
                read = both[0 : 2 * rows] + both[2 * rows :] + dot(high, state_low)
                for j in range(group):
                    to = (g * group + j) * rows
                    lanes = slice(j * LANES, (j + 1) * LANES)
                    sent[part, to : to + rows] = read[rows:, lanes]
                    to += heads * rows
                    sent[part, to : to + rows] = read[0:rows, lanes]
            to = 2 * heads * rows
            sent[part, to : to + SUB] = pltpu.roll(sums[...], (LANES - p * rows) % LANES, 1)
            sent_copy(part).start()

    outputs = [
        pltpu.make_async_copy(keys_all, keys_hbm, out_sems.at[0]),
        pltpu.make_async_copy(decay_all, decay_hbm, out_sems.at[1]),
    ]
    for copy in outputs:
        copy.start()

    @pl.loop(0, parts)
    def _(part):
        sent_copy(part).wait()

    for copy in outputs:
        copy.wait()


def owner_kernel(arrived, values, zgate, decay, beta, norm_gain, delta_out, normed_out):
    rows, heads = decay.shape
    key_heads = 2
    group = heads // key_heads
    total = arrived[0]
    for n in range(1, arrived.shape[0]):
        total = total + arrived[n]
    sums = jnp.transpose(total[2 * heads * rows :])[0:rows]
    query_scale = lax.rsqrt(1.0 + sums[:, 0:key_heads])
    key_scale = lax.rsqrt(1.0 + sums[:, key_heads : 2 * key_heads])
    unit_dot = sums[:, 2 * key_heads : 3 * key_heads] * query_scale * key_scale
    for h in range(heads):
        g = h // group
        lanes = slice(h * LANES, (h + 1) * LANES)
        d = decay[:, h : h + 1]
        ks = key_scale[:, g : g + 1]
        readk = total[h * rows : (h + 1) * rows] * ks
        delta = beta[:, h : h + 1] * (values[:, lanes] - d * readk)
        raw_q = total[(heads + h) * rows : (heads + h + 1) * rows]
        readq = d * (raw_q * query_scale[:, g : g + 1]) + unit_dot[:, g : g + 1] * delta
        meansq = jnp.mean(readq * readq, axis=1, keepdims=True)
        z = zgate[:, lanes]
        normed = readq * lax.rsqrt(meansq + 0.5) * norm_gain[...] * (z / (1.0 + jnp.exp(-z)))
        normed_out[:, lanes] = normed.astype(jnp.bfloat16)
        scaled = delta * ks
        for n in range(delta_out.shape[0]):
            delta_out[n, h * rows : (h + 1) * rows] = scaled


def update_kernel(delta, keys_hbm, decay_hbm, state_hbm, new_state, keys, decay, wide, state, ready, small_sems, in_sems, out_sems):
    parts, rows, heads = state.shape[0:3]
    key_heads = keys.shape[0] // SUB
    group = heads // key_heads
    span = rows * SUB
    per_tile = LANES // rows
    together = 4

    small = [
        pltpu.make_async_copy(decay_hbm, decay, small_sems.at[0]),
        pltpu.make_async_copy(keys_hbm, keys, small_sems.at[1]),
    ]
    for copy in small:
        copy.start()

    def read(n):
        return pltpu.make_async_copy(state_hbm.at[pl.ds(n * rows, rows)], state.at[n], in_sems.at[n])

    def write(n):
        return pltpu.make_async_copy(ready.at[n], new_state.at[pl.ds(n * rows, rows)], out_sems.at[n])

    ahead = 6
    for n in range(ahead):
        read(n).start()
    lane = lax.broadcasted_iota(jnp.int32, (SUB, LANES), 1)
    slot = lax.broadcasted_iota(jnp.int32, (span, LANES), 1)
    own = (slot % rows == lax.broadcasted_iota(jnp.int32, (span, LANES), 0) // SUB) & (slot < 3 * rows)
    ones = jnp.ones((LANES, LANES), jnp.bfloat16)
    for copy in small:
        copy.wait()

    @pl.loop(0, parts // per_tile)
    def _(n):
        at = pl.multiple_of(n * LANES, LANES)
        some = decay[pl.ds(at, LANES)]
        for h in range(heads):
            spread = jnp.broadcast_to(some[:, h : h + 1], (LANES, LANES)).reshape(per_tile, rows, LANES)
            wide[pl.ds(n * per_tile, per_tile), :, h * LANES : (h + 1) * LANES] = spread

    @pl.loop(0, parts // together)
    def _(pair):
        tile = keys[:, pl.ds(pl.multiple_of(pair * together // per_tile * LANES, LANES), LANES)]
        for n in range(together):
            part = pair * together + n
            key = pltpu.roll(tile, (LANES - part % per_tile * rows) % LANES, 1)
            high = key.astype(jnp.bfloat16).astype(jnp.float32)
            rest = key - high
            middle = rest.astype(jnp.bfloat16).astype(jnp.float32)
            low = pltpu.roll(rest - middle, 2 * rows, 1)
            packed = jnp.where(lane[0:1] < rows, high, jnp.where(lane[0:1] < 2 * rows, pltpu.roll(middle, rows, 1), low))
            read(part).wait()

            @pl.when(part + ahead < parts)
            def _():
                read(part + ahead).start()

            for g in range(key_heads):
                spread = jnp.broadcast_to(packed[None, g * SUB : (g + 1) * SUB], (rows, SUB, LANES)).reshape(span, LANES)
                wide_key = dot(jnp.where(own, spread, 0.0).astype(jnp.bfloat16), ones)
                for b in range(rows):
                    k = wide_key[b * SUB : (b + 1) * SUB]
                    for h in range(g * group, (g + 1) * group):
                        row = jnp.broadcast_to(delta[part, h * rows + b : h * rows + b + 1], (SUB, LANES))
                        factor = jnp.broadcast_to(wide[part, b : b + 1, h * LANES : (h + 1) * LANES], (SUB, LANES))
                        ready[part, b, h] = factor * state[part, b, h] + k * row
            write(part).start()

    @pl.loop(0, parts)
    def _(part):
        write(part).wait()


def project_kernel(core, normed, w_out_hbm, give, keep, w_out, sem):
    copy = pltpu.make_async_copy(w_out_hbm, w_out, sem)
    copy.start()
    copy.wait()
    total = dot(normed[...], w_out[...])
    size = give.shape[2]
    first = core[0] == 0
    for y in range(give.shape[0]):
        even = total[:, 2 * y * size : (2 * y + 1) * size]
        odd = total[:, (2 * y + 1) * size : (2 * y + 2) * size]
        keep[y] = jnp.where(first, even, odd)
        give[y] = jnp.where(first, odd, even)


def chip_kernel(y, keep, got, own, *away):
    size = keep.shape[0]
    own[...] = keep[y[0]] + got[y[0]]
    for n, out in enumerate(away):
        at = (y[0] + n + 1) % size
        out[...] = keep[at] + got[at]


def head_exchange(normed, w_out, y_size):
    rows = normed.shape[0]
    heads = 2 * y_size
    size = w_out.shape[1] // heads
    head = lax.axis_index("head")
    in_smem = pl.BlockSpec(memory_space=pltpu.SMEM)
    in_vmem = pl.BlockSpec(memory_space=pltpu.VMEM)
    limit = pltpu.CompilerParams(vmem_limit_bytes=8 * 1024 * 1024)
    piece = jax.ShapeDtypeStruct((y_size, rows, size), jnp.float32)
    give, keep = pl.pallas_call(
        project_kernel,
        in_specs=[in_smem, in_vmem, pl.BlockSpec(memory_space=pl.ANY)],
        out_specs=[in_vmem, in_vmem],
        out_shape=[piece, piece],
        scratch_shapes=[pltpu.VMEM(w_out.shape, w_out.dtype), pltpu.SemaphoreType.DMA],
        compiler_params=limit,
        name="project_out",
    )((head % 2)[None], normed, pltpu.with_memory_space_constraint(w_out, pltpu.HBM))
    got = lax.ppermute(give, "head", [(h, h ^ 1) for h in range(heads)])
    total, *away = pl.pallas_call(
        chip_kernel,
        in_specs=[in_smem, in_vmem, in_vmem],
        out_specs=[in_vmem] * y_size,
        out_shape=[jax.ShapeDtypeStruct((rows, size), jnp.float32)] * y_size,
        compiler_params=limit,
        name="chip_sum",
    )((head // 2)[None], keep, got)
    for s, part in enumerate(away, 1):
        total = total + lax.ppermute(part, "head", [(h, (h + 2 * s) % heads) for h in range(heads)])
    return total


def decode(
    hidden_in,
    w_query,
    w_key,
    w_value,
    w_zgate,
    w_decay,
    w_beta,
    decay_log,
    dt_bias,
    norm_gain,
    w_out,
    state,
):
    parts = lax.axis_size("row")
    seqs, width = hidden_in.shape
    rows = seqs // parts
    heads = state.shape[1]
    key_rows = w_query.shape[1] * w_query.shape[2]
    per_part = 2 * heads * rows + SUB
    f32 = jnp.float32

    def in_hbm(value):
        return pltpu.with_memory_space_constraint(value, pltpu.HBM)

    any_space = pl.BlockSpec(memory_space=pl.ANY)
    in_vmem = pl.BlockSpec(memory_space=pltpu.VMEM)
    limit = pltpu.CompilerParams(vmem_limit_bytes=20 * 1024 * 1024)
    sent, keys, decay_all = pl.pallas_call(
        read_kernel,
        in_specs=[any_space] * 7,
        out_specs=[any_space] * 3,
        out_shape=[
            pltpu.HBM((parts, per_part, LANES), f32),
            pltpu.HBM((key_rows, seqs), f32),
            pltpu.HBM((seqs, heads), f32),
        ],
        scratch_shapes=[
            pltpu.VMEM((seqs // LANES, LANES, width), jnp.bfloat16),
            pltpu.VMEM((LANES, width), jnp.bfloat16),
            pltpu.VMEM((heads, width), jnp.bfloat16),
            pltpu.VMEM((1, heads), f32),
            pltpu.VMEM((1, heads), f32),
            pltpu.VMEM((parts, rows, heads, SUB, LANES), f32),
            pltpu.VMEM((parts, per_part, LANES), f32),
            pltpu.VMEM((2 * key_rows // SUB, LANES, rows * SUB), jnp.bfloat16),
            pltpu.VMEM((SUB, LANES), f32),
            pltpu.VMEM((key_rows, seqs), f32),
            pltpu.VMEM((seqs, heads), f32),
            pltpu.SemaphoreType.DMA((5,)),
            pltpu.SemaphoreType.DMA((seqs // LANES,)),
            pltpu.SemaphoreType.DMA((parts,)),
            pltpu.SemaphoreType.DMA((parts,)),
            pltpu.SemaphoreType.DMA((2,)),
        ],
        compiler_params=limit,
        name="read_state",
    )(
        in_hbm(hidden_in),
        in_hbm(jnp.transpose(w_query, (1, 2, 0)).reshape(key_rows, width)),
        in_hbm(jnp.transpose(w_key, (1, 2, 0)).reshape(key_rows, width)),
        in_hbm(jnp.transpose(w_decay)),
        in_hbm(decay_log[None]),
        in_hbm(dt_bias[None]),
        in_hbm(state),
    )
    arrived = lax.all_to_all(sent, "row", 0, 0, tiled=True)

    own_hidden = lax.dynamic_slice_in_dim(hidden_in, lax.axis_index("row") * rows, rows, 0)
    values = jnp.einsum("bd,dhv->bhv", own_hidden, w_value, preferred_element_type=f32).reshape(rows, heads * LANES)
    zgate = jnp.einsum("bd,dhv->bhv", own_hidden, w_zgate, preferred_element_type=f32).reshape(rows, heads * LANES)
    decay_in = jnp.dot(own_hidden, w_decay, preferred_element_type=f32) + dt_bias
    decay = jnp.exp(-jnp.exp(decay_log) * jax.nn.softplus(decay_in))
    beta = jax.nn.sigmoid(jnp.dot(own_hidden, w_beta, preferred_element_type=f32))

    delta_own, normed = pl.pallas_call(
        owner_kernel,
        out_shape=[
            pltpu.VMEM((parts, heads * rows, LANES), f32),
            pltpu.VMEM((rows, heads * LANES), jnp.bfloat16),
        ],
        compiler_params=limit,
        name="owner_rows",
    )(arrived, values, zgate, decay, beta, norm_gain[None])
    delta = lax.all_to_all(delta_own, "row", 0, 0, tiled=True)

    layer_out = head_exchange(normed, w_out.reshape(heads * LANES, -1), lax.axis_size("head") // 2).astype(jnp.bfloat16)

    new_state = pl.pallas_call(
        update_kernel,
        in_specs=[in_vmem, any_space, any_space, any_space],
        out_specs=any_space,
        out_shape=pltpu.HBM(state.shape, f32),
        scratch_shapes=[
            pltpu.VMEM((key_rows, seqs), f32),
            pltpu.VMEM((seqs, heads), f32),
            pltpu.VMEM((parts, rows, heads * LANES), f32),
            pltpu.VMEM((parts, rows, heads, SUB, LANES), f32),
            pltpu.VMEM((parts, rows, heads, SUB, LANES), f32),
            pltpu.SemaphoreType.DMA((2,)),
            pltpu.SemaphoreType.DMA((parts,)),
            pltpu.SemaphoreType.DMA((parts,)),
        ],
        compiler_params=pltpu.CompilerParams(vmem_limit_bytes=24 * 1024 * 1024),
        name="update_state",
    )(delta, in_hbm(keys), in_hbm(decay_all), in_hbm(state))
    return (layer_out, new_state)


def solution(mesh):
    in_specs = (
        P(),
        P(None, "head", "row"),
        P(None, "head", "row"),
        P(None, "head", None),
        P(None, "head", None),
        P(None, "head"),
        P(None, "head"),
        P("head"),
        P("head"),
        P(),
        P("head", None, None),
        P(None, "head", "row", None),
    )
    out_specs = (P("row", "head"), P(None, "head", "row", None))
    return jax.shard_map(decode, mesh=mesh, in_specs=in_specs, out_specs=out_specs, check_vma=False)
```

```python
import jax
import jax.numpy as jnp
from jax import lax
from jax.experimental import pallas as pl
from jax.experimental.pallas import tpu as pltpu
from jax.sharding import PartitionSpec as P


LANES = 128
SUB = 8
BLOCK = 16
SIDE = 4


def high_low(value):
    high = value.astype(jnp.bfloat16)
    return high, (value - high.astype(jnp.float32)).astype(jnp.bfloat16)


def dot(left, right):
    return jnp.dot(left, right, preferred_element_type=jnp.float32)


def read_kernel(
    hidden_hbm,
    w_query_hbm,
    w_key_hbm,
    w_decay_hbm,
    decay_log_hbm,
    dt_bias_hbm,
    state_hbm,
    *rest,
):
    by_x, by_z = rest[0:SIDE], rest[SIDE : 2 * SIDE]
    keys_hbm, decay_hbm, hidden, weights, w_decay, decay_log, dt_bias, state = rest[2 * SIDE : 2 * SIDE + 8]
    reads_k, reads_q, left, picks, sums, keys_all, decay_all = rest[2 * SIDE + 8 : 2 * SIDE + 15]
    in_sems, hidden_sems, state_sems, k_sems, q_sems, out_sems = rest[2 * SIDE + 15 :]
    me = lax.axis_index("row")
    my_x, my_z = me // SIDE, me % SIDE
    parts, rows, heads = state.shape[0:3]
    chunks = hidden.shape[0]
    blocks = LANES // BLOCK
    key_rows = w_query_hbm.shape[0]
    key_heads = key_rows // SUB
    group = heads // key_heads
    few = BLOCK
    span = few * SUB
    pad = weights.dtype.itemsize * SUB

    inputs = [
        pltpu.make_async_copy(w_query_hbm, weights.at[pad : pad + key_rows], in_sems.at[0]),
        pltpu.make_async_copy(w_key_hbm, weights.at[pad + key_rows : pad + 2 * key_rows], in_sems.at[1]),
        pltpu.make_async_copy(w_decay_hbm, w_decay, in_sems.at[2]),
        pltpu.make_async_copy(decay_log_hbm, decay_log, in_sems.at[3]),
        pltpu.make_async_copy(dt_bias_hbm, dt_bias, in_sems.at[4]),
    ]
    for copy in inputs:
        copy.start()

    def chunk_of(s):
        return (my_x + s) % SIDE

    def hidden_copy(s):
        at = pl.multiple_of(chunk_of(s) * LANES, LANES)
        return pltpu.make_async_copy(hidden_hbm.at[pl.ds(at, LANES)], hidden.at[s], hidden_sems.at[s])

    def state_copy(n):
        part = chunk_of(n // SIDE) * SIDE + (my_z + n % SIDE) % SIDE
        return pltpu.make_async_copy(state_hbm.at[pl.ds(part * rows, rows)], state.at[n], state_sems.at[n])

    def k_copy(s, to):
        return pltpu.make_async_copy(reads_k.at[s], to, k_sems.at[s])

    def q_copy(s, t):
        return pltpu.make_async_copy(reads_q.at[s, t], by_z[t].at[s], q_sems.at[s, t])

    ahead = 8
    for n in range(chunks):
        hidden_copy(n).start()
    width = weights.shape[1]
    weights[0:pad] = jnp.zeros((pad, width), weights.dtype)
    weights[pad + 2 * key_rows :] = jnp.zeros((LANES - pad - 2 * key_rows, width), weights.dtype)
    sums[...] = jnp.zeros(sums.shape, sums.dtype)
    source = lax.broadcasted_iota(jnp.int32, (LANES, span), 0)
    entry = lax.broadcasted_iota(jnp.int32, (LANES, span), 1) % SUB
    own = lax.broadcasted_iota(jnp.int32, (few, span), 1) // SUB == lax.broadcasted_iota(jnp.int32, (few, span), 0)
    for n in range(2 * key_heads):
        picks[n] = (source == pad + n * SUB + entry).astype(jnp.bfloat16)
    for copy in inputs:
        copy.wait()
    weights[0:heads] = w_decay[...]

    @pl.loop(0, chunks)
    def _(s):
        chunk = chunk_of(s)
        hidden_copy(s).wait()

        @pl.when(s == 0)
        def _():
            for n in range(ahead):
                state_copy(n).start()

        projected = lax.dot_general(hidden[s], weights[...], (((1,), (1,)), ((), ())), preferred_element_type=jnp.float32)
        halves = jnp.concatenate(high_low(projected), axis=0)
        for n in range(2 * key_heads):
            wide = dot(halves, picks[n]).reshape(2 * blocks, few, span)
            left[n] = jnp.where(own[None], wide, 0.0).astype(jnp.bfloat16)

        at = pl.multiple_of(chunk * LANES, LANES)
        pre = projected[:, 0:heads] + dt_bias[...]
        soft = jnp.maximum(pre, 0.0) + jnp.log1p(jnp.exp(-jnp.abs(pre)))
        decay_all[pl.ds(at, LANES)] = jnp.exp(-jnp.exp(decay_log[...]) * soft)
        turned = jnp.transpose(projected)
        query = turned[pad : pad + key_rows]
        keys = turned[pad + key_rows : pad + 2 * key_rows]
        keys_all[:, pl.ds(at, LANES)] = keys
        for n, product in enumerate((query * query, keys * keys, query * keys)):
            for g in range(key_heads):
                sums[n * key_heads + g : n * key_heads + g + 1] = jnp.sum(product[g * SUB : (g + 1) * SUB], axis=0, keepdims=True)

        for t in range(SIDE):
            p = (my_z + t) % SIDE
            turn = s * SIDE + t
            state_copy(turn).wait()

            @pl.when(turn + ahead < parts)
            def _():
                state_copy(turn + ahead).start()

            for first in range(0, rows, few):
                block = p * (rows // few) + first // few
                for g in range(key_heads):
                    tiles = [state[turn, first : first + few, g * group + j].reshape(span, LANES) for j in range(group)]
                    state_high, state_low = high_low(jnp.concatenate(tiles, axis=1))
                    high = jnp.concatenate([left[g, block], left[key_heads + g, block]], axis=0)
                    low = jnp.concatenate([left[g, blocks + block], left[key_heads + g, blocks + block]], axis=0)
                    both = dot(jnp.concatenate([high, low], axis=0), state_high)
                    read = both[0 : 2 * few] + both[2 * few :] + dot(high, state_low)
                    for j in range(group):
                        to = (g * group + j) * rows + first
                        lanes = slice(j * LANES, (j + 1) * LANES)
                        reads_k[s, t, to : to + few] = read[few:, lanes]
                        reads_q[s, t, to : to + few] = read[0:few, lanes]
            reads_q[s, t, heads * rows :] = pltpu.roll(sums[...], (LANES - p * rows) % LANES, 1)
            q_copy(s, t).start()
        for k in range(SIDE):

            @pl.when(s == k)
            def _():
                k_copy(s, by_x[k]).start()

    outputs = [
        pltpu.make_async_copy(keys_all, keys_hbm, out_sems.at[0]),
        pltpu.make_async_copy(decay_all, decay_hbm, out_sems.at[1]),
    ]
    for copy in outputs:
        copy.start()

    for k in range(SIDE):
        k_copy(k, by_x[k]).wait()
        for t in range(SIDE):
            q_copy(k, t).wait()
    for copy in outputs:
        copy.wait()


def owner_kernel(*refs):
    arrived = refs[0 : 2 * SIDE]
    values, zgate, decay, beta, norm_gain, delta_hbm, normed_out, scaled, out_sems = refs[2 * SIDE :]
    rows, heads = decay.shape
    parts = delta_hbm.shape[0]
    key_heads = 2
    group = heads // key_heads
    read_k, read_q = ((x[0][...] + x[1][...]) + (x[2][...] + x[3][...]) for x in (arrived[0:SIDE], arrived[SIDE:]))
    sums = jnp.transpose(read_q[heads * rows :])[0:rows]
    query_scale = lax.rsqrt(1.0 + sums[:, 0:key_heads])
    key_scale = lax.rsqrt(1.0 + sums[:, key_heads : 2 * key_heads])
    unit_dot = sums[:, 2 * key_heads : 3 * key_heads] * query_scale * key_scale
    reads = []
    for h in range(heads):
        g = h // group
        lanes = slice(h * LANES, (h + 1) * LANES)
        d = decay[:, h : h + 1]
        ks = key_scale[:, g : g + 1]
        readk = read_k[h * rows : (h + 1) * rows] * ks
        delta = beta[:, h : h + 1] * (values[:, lanes] - d * readk)
        raw_q = read_q[h * rows : (h + 1) * rows]
        scaled[h * rows : (h + 1) * rows] = delta * ks
        reads.append(d * (raw_q * query_scale[:, g : g + 1]) + unit_dot[:, g : g + 1] * delta)
    outputs = [pltpu.make_async_copy(scaled, delta_hbm.at[n], out_sems.at[n]) for n in range(parts)]
    for copy in outputs:
        copy.start()
    for h, readq in enumerate(reads):
        lanes = slice(h * LANES, (h + 1) * LANES)
        meansq = jnp.mean(readq * readq, axis=1, keepdims=True)
        z = zgate[:, lanes]
        normed = readq * lax.rsqrt(meansq + 0.5) * norm_gain[...] * (z / (1.0 + jnp.exp(-z)))
        normed_out[:, lanes] = normed.astype(jnp.bfloat16)
    for copy in outputs:
        copy.wait()


def update_kernel(delta, keys_hbm, decay_hbm, state_hbm, new_state, keys, decay, wide, state, ready, small_sems, in_sems, out_sems):
    parts, rows, heads = state.shape[0:3]
    key_heads = keys.shape[0] // SUB
    group = heads // key_heads
    few = BLOCK
    span = few * SUB
    per_tile = LANES // rows

    small = [
        pltpu.make_async_copy(decay_hbm, decay, small_sems.at[0]),
        pltpu.make_async_copy(keys_hbm, keys, small_sems.at[1]),
    ]
    for copy in small:
        copy.start()

    def read(n):
        return pltpu.make_async_copy(state_hbm.at[pl.ds(n * rows, rows)], state.at[n], in_sems.at[n])

    def write(n):
        return pltpu.make_async_copy(ready.at[n], new_state.at[pl.ds(n * rows, rows)], out_sems.at[n])

    ahead = 6
    for n in range(ahead):
        read(n).start()
    lane = lax.broadcasted_iota(jnp.int32, (SUB, LANES), 1)
    slot = lax.broadcasted_iota(jnp.int32, (span, LANES), 1)
    own = (slot % few == lax.broadcasted_iota(jnp.int32, (span, LANES), 0) // SUB) & (slot < 3 * few)
    ones = jnp.ones((LANES, LANES), jnp.bfloat16)
    for copy in small:
        copy.wait()

    @pl.loop(0, parts // per_tile)
    def _(n):
        at = pl.multiple_of(n * LANES, LANES)
        some = decay[pl.ds(at, LANES)]
        for h in range(heads):
            spread = jnp.broadcast_to(some[:, h : h + 1], (LANES, LANES)).reshape(per_tile, rows, LANES)
            wide[pl.ds(n * per_tile, per_tile), :, h * LANES : (h + 1) * LANES] = spread

    @pl.loop(0, parts // per_tile)
    def _(tile):
        raw = keys[:, pl.ds(pl.multiple_of(tile * LANES, LANES), LANES)]
        high = raw.astype(jnp.bfloat16).astype(jnp.float32)
        rest = raw - high
        middle = rest.astype(jnp.bfloat16).astype(jnp.float32)
        low = rest - middle
        for n in range(per_tile):
            part = tile * per_tile + n
            read(part).wait()

            @pl.when(part + ahead < parts)
            def _():
                read(part + ahead).start()

            for first in range(0, rows, few):
                back = LANES - n * rows - first
                turned = [pltpu.roll(x, (back + m * few) % LANES, 1) for m, x in enumerate((high, middle, low))]
                packed = jnp.where(lane[0:1] < few, turned[0], jnp.where(lane[0:1] < 2 * few, turned[1], turned[2]))
                for g in range(key_heads):
                    spread = jnp.broadcast_to(packed[None, g * SUB : (g + 1) * SUB], (few, SUB, LANES)).reshape(span, LANES)
                    wide_key = dot(jnp.where(own, spread, 0.0).astype(jnp.bfloat16), ones)
                    for b in range(few):
                        k = wide_key[b * SUB : (b + 1) * SUB]
                        at = first + b
                        for h in range(g * group, (g + 1) * group):
                            row = jnp.broadcast_to(delta[part, h * rows + at : h * rows + at + 1], (SUB, LANES))
                            factor = jnp.broadcast_to(wide[part, at : at + 1, h * LANES : (h + 1) * LANES], (SUB, LANES))
                            ready[part, at, h] = factor * state[part, at, h] + k * row
            write(part).start()

    @pl.loop(0, parts)
    def _(part):
        write(part).wait()


def project_kernel(core, normed, w_out_hbm, give, keep, w_out, sem):
    copy = pltpu.make_async_copy(w_out_hbm, w_out, sem)
    copy.start()
    copy.wait()
    total = dot(normed[...], w_out[...])
    size = give.shape[2]
    first = core[0] == 0
    for y in range(give.shape[0]):
        even = total[:, 2 * y * size : (2 * y + 1) * size]
        odd = total[:, (2 * y + 1) * size : (2 * y + 2) * size]
        keep[y] = jnp.where(first, even, odd)
        give[y] = jnp.where(first, odd, even)


def chip_kernel(y, keep, got, own, *away):
    size = keep.shape[0]
    own[...] = keep[y[0]] + got[y[0]]
    for n, out in enumerate(away):
        at = (y[0] + n + 1) % size
        out[...] = keep[at] + got[at]


def head_exchange(normed, w_out, y_size):
    rows = normed.shape[0]
    heads = 2 * y_size
    size = w_out.shape[1] // heads
    head = lax.axis_index("head")
    in_smem = pl.BlockSpec(memory_space=pltpu.SMEM)
    in_vmem = pl.BlockSpec(memory_space=pltpu.VMEM)
    limit = pltpu.CompilerParams(vmem_limit_bytes=8 * 1024 * 1024)
    piece = jax.ShapeDtypeStruct((y_size, rows, size), jnp.float32)
    give, keep = pl.pallas_call(
        project_kernel,
        in_specs=[in_smem, in_vmem, pl.BlockSpec(memory_space=pl.ANY)],
        out_specs=[in_vmem, in_vmem],
        out_shape=[piece, piece],
        scratch_shapes=[pltpu.VMEM(w_out.shape, w_out.dtype), pltpu.SemaphoreType.DMA],
        compiler_params=limit,
        name="project_out",
    )((head % 2)[None], normed, pltpu.with_memory_space_constraint(w_out, pltpu.HBM))
    got = lax.ppermute(give, "head", [(h, h ^ 1) for h in range(heads)])
    total, *away = pl.pallas_call(
        chip_kernel,
        in_specs=[in_smem, in_vmem, in_vmem],
        out_specs=[in_vmem] * y_size,
        out_shape=[jax.ShapeDtypeStruct((rows, size), jnp.float32)] * y_size,
        compiler_params=limit,
        name="chip_sum",
    )((head // 2)[None], keep, got)
    for s, part in enumerate(away, 1):
        total = total + lax.ppermute(part, "head", [(h, (h + 2 * s) % heads) for h in range(heads)])
    return total


def decode(
    hidden_in,
    w_query,
    w_key,
    w_value,
    w_zgate,
    w_decay,
    w_beta,
    decay_log,
    dt_bias,
    norm_gain,
    w_out,
    state,
):
    parts = lax.axis_size("row")
    seqs, width = hidden_in.shape
    rows = seqs // parts
    heads = state.shape[1]
    key_rows = w_query.shape[1] * w_query.shape[2]
    f32 = jnp.float32

    def in_hbm(value):
        return pltpu.with_memory_space_constraint(value, pltpu.HBM)

    any_space = pl.BlockSpec(memory_space=pl.ANY)
    in_vmem = pl.BlockSpec(memory_space=pltpu.VMEM)
    limit = pltpu.CompilerParams(vmem_limit_bytes=20 * 1024 * 1024)
    extra = heads * rows + SUB
    per_k, per_q = (SIDE, heads * rows, LANES), (SIDE, extra, LANES)
    *sent, keys, decay_all = pl.pallas_call(
        read_kernel,
        in_specs=[any_space] * 7,
        out_specs=[in_vmem] * (2 * SIDE) + [any_space] * 2,
        out_shape=[pltpu.VMEM(per_k, f32)] * SIDE
        + [pltpu.VMEM(per_q, f32)] * SIDE
        + [pltpu.HBM((key_rows, seqs), f32), pltpu.HBM((seqs, heads), f32)],
        scratch_shapes=[
            pltpu.VMEM((seqs // LANES, LANES, width), jnp.bfloat16),
            pltpu.VMEM((LANES, width), jnp.bfloat16),
            pltpu.VMEM((heads, width), jnp.bfloat16),
            pltpu.VMEM((1, heads), f32),
            pltpu.VMEM((1, heads), f32),
            pltpu.VMEM((parts, rows, heads, SUB, LANES), f32),
            pltpu.VMEM((SIDE, *per_k), f32),
            pltpu.VMEM((SIDE, *per_q), f32),
            pltpu.VMEM((2 * key_rows // SUB, 2 * LANES // BLOCK, BLOCK, BLOCK * SUB), jnp.bfloat16),
            pltpu.VMEM((2 * key_rows // SUB, LANES, BLOCK * SUB), jnp.bfloat16),
            pltpu.VMEM((SUB, LANES), f32),
            pltpu.VMEM((key_rows, seqs), f32),
            pltpu.VMEM((seqs, heads), f32),
            pltpu.SemaphoreType.DMA((5,)),
            pltpu.SemaphoreType.DMA((seqs // LANES,)),
            pltpu.SemaphoreType.DMA((parts,)),
            pltpu.SemaphoreType.DMA((SIDE,)),
            pltpu.SemaphoreType.DMA((SIDE, SIDE)),
            pltpu.SemaphoreType.DMA((2,)),
        ],
        compiler_params=limit,
        name="read_state",
    )(
        in_hbm(hidden_in),
        in_hbm(jnp.transpose(w_query, (1, 2, 0)).reshape(key_rows, width)),
        in_hbm(jnp.transpose(w_key, (1, 2, 0)).reshape(key_rows, width)),
        in_hbm(jnp.transpose(w_decay)),
        in_hbm(decay_log[None]),
        in_hbm(dt_bias[None]),
        in_hbm(state),
    )

    def along_x(value, step):
        return lax.ppermute(value, "row", [(n, (n + SIDE * step) % parts) for n in range(parts)])

    def along_z(value, step):
        return lax.ppermute(value, "row", [(n, n // SIDE * SIDE + (n + step) % SIDE) for n in range(parts)])

    steps = (1, 3, 2)
    got_k = [along_x(sent[n], n) for n in steps]
    got_q = [along_z(sent[SIDE + n], n) for n in steps]
    part_k, part_q = (
        [(own[n] + got[0][n]) + (got[1][n] + got[2][n]) for n in range(SIDE)]
        for own, got in ((sent[0], got_k), (sent[SIDE], got_q))
    )
    arrived = [part_k[0], *(along_z(part_k[n], n) for n in steps)]
    arrived += [part_q[0], *(along_x(part_q[n], n) for n in steps)]

    own_hidden = lax.dynamic_slice_in_dim(hidden_in, lax.axis_index("row") * rows, rows, 0)
    values = jnp.einsum("bd,dhv->bhv", own_hidden, w_value, preferred_element_type=f32).reshape(rows, heads * LANES)
    zgate = jnp.einsum("bd,dhv->bhv", own_hidden, w_zgate, preferred_element_type=f32).reshape(rows, heads * LANES)
    decay_in = jnp.dot(own_hidden, w_decay, preferred_element_type=f32) + dt_bias
    decay = jnp.exp(-jnp.exp(decay_log) * jax.nn.softplus(decay_in))
    beta = jax.nn.sigmoid(jnp.dot(own_hidden, w_beta, preferred_element_type=f32))

    delta_own, normed = pl.pallas_call(
        owner_kernel,
        in_specs=[in_vmem] * (2 * SIDE + 5),
        out_specs=[any_space, in_vmem],
        out_shape=[
            pltpu.HBM((parts, heads * rows, LANES), f32),
            pltpu.VMEM((rows, heads * LANES), jnp.bfloat16),
        ],
        scratch_shapes=[
            pltpu.VMEM((heads * rows, LANES), f32),
            pltpu.SemaphoreType.DMA((parts,)),
        ],
        compiler_params=limit,
        name="owner_rows",
    )(*arrived, values, zgate, decay, beta, norm_gain[None])
    delta = lax.all_to_all(delta_own, "row", 0, 0, tiled=True)

    layer_out = head_exchange(normed, w_out.reshape(heads * LANES, -1), lax.axis_size("head") // 2).astype(jnp.bfloat16)

    new_state = pl.pallas_call(
        update_kernel,
        in_specs=[in_vmem, any_space, any_space, any_space],
        out_specs=any_space,
        out_shape=pltpu.HBM(state.shape, f32),
        scratch_shapes=[
            pltpu.VMEM((key_rows, seqs), f32),
            pltpu.VMEM((seqs, heads), f32),
            pltpu.VMEM((parts, rows, heads * LANES), f32),
            pltpu.VMEM((parts, rows, heads, SUB, LANES), f32),
            pltpu.VMEM((parts, rows, heads, SUB, LANES), f32),
            pltpu.SemaphoreType.DMA((2,)),
            pltpu.SemaphoreType.DMA((parts,)),
            pltpu.SemaphoreType.DMA((parts,)),
        ],
        compiler_params=pltpu.CompilerParams(vmem_limit_bytes=24 * 1024 * 1024),
        name="update_state",
    )(delta, in_hbm(keys), in_hbm(decay_all), in_hbm(state))
    return (layer_out, new_state)


def solution(mesh):
    in_specs = (
        P(),
        P(None, "head", "row"),
        P(None, "head", "row"),
        P(None, "head", None),
        P(None, "head", None),
        P(None, "head"),
        P(None, "head"),
        P("head"),
        P("head"),
        P(),
        P("head", None, None),
        P(None, "head", "row", None),
    )
    out_specs = (P("row", "head"), P(None, "head", "row", None))
    return jax.shard_map(decode, mesh=mesh, in_specs=in_specs, out_specs=out_specs, check_vma=False)
```

```python
import jax
import jax.numpy as jnp
from jax import lax
from jax.experimental import pallas as pl
from jax.experimental.pallas import tpu as pltpu
from jax.sharding import PartitionSpec as P


LANES = 128
SUB = 8
BLOCK = 16
SIDE = 4
KEY_HEADS = 2


def high_low(value):
    high = value.astype(jnp.bfloat16)
    return high, (value - high.astype(jnp.float32)).astype(jnp.bfloat16)


def dot(left, right):
    return jnp.dot(left, right, preferred_element_type=jnp.float32)


def read_kernel(
    hidden_hbm,
    w_query_hbm,
    w_key_hbm,
    w_decay_hbm,
    w_beta_hbm,
    decay_log_hbm,
    dt_bias_hbm,
    state_hbm,
    *rest,
):
    by_x, by_z = rest[0:SIDE], rest[SIDE : 2 * SIDE]
    keys_hbm, decay_hbm, decay_own, beta_own = rest[2 * SIDE : 2 * SIDE + 4]
    hidden, weights, w_decay, w_beta, decay_log, dt_bias, state = rest[2 * SIDE + 4 : 2 * SIDE + 11]
    reads_k, left, picks, sums, keys_all, decay_all, beta_all = rest[2 * SIDE + 11 : 2 * SIDE + 18]
    in_sems, hidden_sems, state_sems, k_sems, out_sems = rest[2 * SIDE + 18 :]
    me = lax.axis_index("row")
    my_x, my_z = me // SIDE, me % SIDE
    _, rows, heads = state.shape[0:3]
    chunks = hidden.shape[0]
    blocks = LANES // BLOCK
    key_rows = w_query_hbm.shape[0]
    key_heads = key_rows // SUB
    group = heads // key_heads
    few = BLOCK
    span = few * SUB
    pad = weights.dtype.itemsize * SUB

    inputs = [
        pltpu.make_async_copy(w_query_hbm, weights.at[pad : pad + key_rows], in_sems.at[0]),
        pltpu.make_async_copy(w_key_hbm, weights.at[pad + key_rows : pad + 2 * key_rows], in_sems.at[1]),
        pltpu.make_async_copy(w_decay_hbm, w_decay, in_sems.at[2]),
        pltpu.make_async_copy(decay_log_hbm, decay_log, in_sems.at[3]),
        pltpu.make_async_copy(dt_bias_hbm, dt_bias, in_sems.at[4]),
        pltpu.make_async_copy(w_beta_hbm, w_beta, in_sems.at[5]),
    ]
    for copy in inputs:
        copy.start()

    def chunk_of(s):
        return (my_x + s) % SIDE

    def hidden_copy(s):
        at = pl.multiple_of(chunk_of(s) * LANES, LANES)
        return pltpu.make_async_copy(hidden_hbm.at[pl.ds(at, LANES)], hidden.at[s], hidden_sems.at[s])

    def state_copy(n):
        part = chunk_of(n // SIDE) * SIDE + (my_z + n % SIDE) % SIDE
        return pltpu.make_async_copy(state_hbm.at[pl.ds(part * rows, rows)], state.at[n], state_sems.at[n])

    def k_copy(s, to):
        return pltpu.make_async_copy(reads_k.at[s], to, k_sems.at[s])

    ahead = 2
    for n in range(ahead):
        hidden_copy(n).start()
    width = weights.shape[1]
    weights[0:pad] = jnp.zeros((pad, width), weights.dtype)
    weights[pad + 2 * key_rows :] = jnp.zeros((LANES - pad - 2 * key_rows, width), weights.dtype)
    sums[...] = jnp.zeros(sums.shape, sums.dtype)
    source = lax.broadcasted_iota(jnp.int32, (LANES, span), 0)
    entry = lax.broadcasted_iota(jnp.int32, (LANES, span), 1) % SUB
    own = lax.broadcasted_iota(jnp.int32, (few, span), 1) // SUB == lax.broadcasted_iota(jnp.int32, (few, span), 0)
    for n in range(2 * key_heads):
        picks[n] = (source == pad + n * SUB + entry).astype(jnp.bfloat16)
    for copy in inputs:
        copy.wait()
    weights[0:heads] = w_decay[...]
    weights[heads : 2 * heads] = w_beta[...]
    for n in range(ahead * SIDE):
        state_copy(n).start()
        if n % SIDE == 1:
            hidden_copy(ahead + n // SIDE).start()

    @pl.loop(0, chunks)
    def _(s):
        chunk = chunk_of(s)
        hidden_copy(s).wait()

        @pl.when(s + ahead < SIDE)
        def _():
            for t in range(SIDE):
                state_copy((s + ahead) * SIDE + t).start()

        projected = lax.dot_general(hidden[s], weights[...], (((1,), (1,)), ((), ())), preferred_element_type=jnp.float32)
        halves = jnp.concatenate(high_low(projected), axis=0)
        for n in range(2 * key_heads):
            wide = dot(halves, picks[n]).reshape(2 * blocks, few, span)
            left[n] = jnp.where(own[None], wide, 0.0).astype(jnp.bfloat16)

        at = pl.multiple_of(chunk * LANES, LANES)
        pre = projected[:, 0:heads] + dt_bias[...]
        soft = jnp.maximum(pre, 0.0) + jnp.log1p(jnp.exp(-jnp.abs(pre)))
        decay_all[pl.ds(at, LANES)] = jnp.exp(-jnp.exp(decay_log[...]) * soft)
        beta_all[pl.ds(at, LANES)] = 1.0 / (1.0 + jnp.exp(-projected[:, heads : 2 * heads]))
        turned = jnp.transpose(projected)
        query = turned[pad : pad + key_rows]
        keys = turned[pad + key_rows : pad + 2 * key_rows]
        keys_all[:, pl.ds(at, LANES)] = keys
        for n, product in enumerate((query * query, keys * keys, query * keys)):
            for g in range(key_heads):
                sums[n * key_heads + g : n * key_heads + g + 1] = jnp.sum(product[g * SUB : (g + 1) * SUB], axis=0, keepdims=True)

        for t in range(SIDE):
            p = (my_z + t) % SIDE
            turn = s * SIDE + t
            state_copy(turn).wait()
            for first in range(0, rows, few):
                block = p * (rows // few) + first // few
                for g in range(key_heads):
                    tiles = [state[turn, first : first + few, g * group + j].reshape(span, LANES) for j in range(group)]
                    state_high, state_low = high_low(jnp.concatenate(tiles, axis=1))
                    high = jnp.concatenate([left[g, block], left[key_heads + g, block]], axis=0)
                    low = jnp.concatenate([left[g, blocks + block], left[key_heads + g, blocks + block]], axis=0)
                    both = dot(jnp.concatenate([high, low], axis=0), state_high)
                    read = both[0 : 2 * few] + both[2 * few :] + dot(high, state_low)
                    for j in range(group):
                        to = (g * group + j) * rows + first
                        lanes = slice(j * LANES, (j + 1) * LANES)
                        reads_k[s, t, to : to + few] = read[few:, lanes]
                        by_z[t][s, to : to + few] = read[0:few, lanes]
            reads_k[s, t, heads * rows :] = pltpu.roll(sums[...], (LANES - p * rows) % LANES, 1)
        for k in range(SIDE):

            @pl.when(s == k)
            def _():
                k_copy(s, by_x[k]).start()

    outputs = [
        pltpu.make_async_copy(keys_all, keys_hbm, out_sems.at[0]),
        pltpu.make_async_copy(decay_all, decay_hbm, out_sems.at[1]),
    ]
    for copy in outputs:
        copy.start()

    mine = pl.ds(pl.multiple_of(me * rows, rows), rows)
    decay_own[...] = decay_all[mine]
    beta_own[...] = beta_all[mine]
    for k in range(SIDE):
        k_copy(k, by_x[k]).wait()
    for copy in outputs:
        copy.wait()


def arrived_sum(parts):
    return (parts[0][...] + parts[1][...]) + (parts[2][...] + parts[3][...])


def delta_kernel(*refs):
    values, decay, beta, delta_hbm, delta_out, scaled, out_sems = refs[SIDE:]
    rows, heads = decay.shape
    parts = delta_hbm.shape[0]
    read_k = arrived_sum(refs[0:SIDE])
    raw_sums = read_k[heads * rows :]
    delta_out[heads * rows :] = raw_sums
    sums = jnp.transpose(raw_sums)[0:rows]
    group = heads // KEY_HEADS
    key_scale = lax.rsqrt(1.0 + sums[:, KEY_HEADS : 2 * KEY_HEADS])
    for h in range(heads):
        g = h // group
        at = slice(h * rows, (h + 1) * rows)
        ks = key_scale[:, g : g + 1]
        readk = read_k[at] * ks
        delta = beta[:, h : h + 1] * (values[h] - decay[:, h : h + 1] * readk)
        delta_out[at] = delta
        scaled[at] = delta * ks
    outputs = [pltpu.make_async_copy(scaled, delta_hbm.at[n], out_sems.at[n]) for n in range(parts)]
    for copy in outputs:
        copy.start()
    for copy in outputs:
        copy.wait()


def norm_kernel(*refs):
    deltas, zgate, decay, norm_gain, normed_out = refs[SIDE:]
    rows, heads = decay.shape
    read_q = arrived_sum(refs[0:SIDE])
    sums = jnp.transpose(deltas[heads * rows :])[0:rows]
    group = heads // KEY_HEADS
    query_scale = lax.rsqrt(1.0 + sums[:, 0:KEY_HEADS])
    key_scale = lax.rsqrt(1.0 + sums[:, KEY_HEADS : 2 * KEY_HEADS])
    unit_dot = sums[:, 2 * KEY_HEADS : 3 * KEY_HEADS] * query_scale * key_scale
    for h in range(heads):
        g = h // group
        lanes = slice(h * LANES, (h + 1) * LANES)
        at = slice(h * rows, (h + 1) * rows)
        readq = decay[:, h : h + 1] * (read_q[at] * query_scale[:, g : g + 1]) + unit_dot[:, g : g + 1] * deltas[at]
        meansq = jnp.mean(readq * readq, axis=1, keepdims=True)
        z = zgate[h]
        normed = readq * lax.rsqrt(meansq + 0.5) * norm_gain[...] * (z / (1.0 + jnp.exp(-z)))
        normed_out[:, lanes] = normed.astype(jnp.bfloat16)


def update_kernel(delta, keys_hbm, decay_hbm, state_hbm, new_state, keys, decay, wide, state, ready, small_sems, in_sems, out_sems):
    parts, rows, heads = state.shape[0:3]
    key_heads = keys.shape[0] // SUB
    group = heads // key_heads
    few = BLOCK
    span = few * SUB
    per_tile = LANES // rows

    small = [
        pltpu.make_async_copy(decay_hbm, decay, small_sems.at[0]),
        pltpu.make_async_copy(keys_hbm, keys, small_sems.at[1]),
    ]
    for copy in small:
        copy.start()

    def read(n):
        return pltpu.make_async_copy(state_hbm.at[pl.ds(n * rows, rows)], state.at[n], in_sems.at[n])

    def write(n):
        return pltpu.make_async_copy(ready.at[n], new_state.at[pl.ds(n * rows, rows)], out_sems.at[n])

    ahead = 6
    for n in range(ahead):
        read(n).start()
    lane = lax.broadcasted_iota(jnp.int32, (SUB, LANES), 1)
    slot = lax.broadcasted_iota(jnp.int32, (span, LANES), 1)
    own = (slot % few == lax.broadcasted_iota(jnp.int32, (span, LANES), 0) // SUB) & (slot < 3 * few)
    ones = jnp.ones((LANES, LANES), jnp.bfloat16)
    for copy in small:
        copy.wait()

    @pl.loop(0, parts // per_tile)
    def _(n):
        at = pl.multiple_of(n * LANES, LANES)
        some = decay[pl.ds(at, LANES)]
        for h in range(heads):
            spread = jnp.broadcast_to(some[:, h : h + 1], (LANES, LANES)).reshape(per_tile, rows, LANES)
            wide[pl.ds(n * per_tile, per_tile), :, h * LANES : (h + 1) * LANES] = spread

    @pl.loop(0, parts // per_tile)
    def _(tile):
        raw = keys[:, pl.ds(pl.multiple_of(tile * LANES, LANES), LANES)]
        high = raw.astype(jnp.bfloat16).astype(jnp.float32)
        rest = raw - high
        middle = rest.astype(jnp.bfloat16).astype(jnp.float32)
        low = rest - middle
        for n in range(per_tile):
            part = tile * per_tile + n
            read(part).wait()

            @pl.when(part + ahead < parts)
            def _():
                read(part + ahead).start()

            for first in range(0, rows, few):
                back = LANES - n * rows - first
                turned = [pltpu.roll(x, (back + m * few) % LANES, 1) for m, x in enumerate((high, middle, low))]
                packed = jnp.where(lane[0:1] < few, turned[0], jnp.where(lane[0:1] < 2 * few, turned[1], turned[2]))
                for g in range(key_heads):
                    spread = jnp.broadcast_to(packed[None, g * SUB : (g + 1) * SUB], (few, SUB, LANES)).reshape(span, LANES)
                    wide_key = dot(jnp.where(own, spread, 0.0).astype(jnp.bfloat16), ones)
                    for b in range(few):
                        k = wide_key[b * SUB : (b + 1) * SUB]
                        at = first + b
                        for h in range(g * group, (g + 1) * group):
                            row = jnp.broadcast_to(delta[part, h * rows + at : h * rows + at + 1], (SUB, LANES))
                            factor = jnp.broadcast_to(wide[part, at : at + 1, h * LANES : (h + 1) * LANES], (SUB, LANES))
                            ready[part, at, h] = factor * state[part, at, h] + k * row
            write(part).start()

    @pl.loop(0, parts)
    def _(part):
        write(part).wait()


def project_kernel(core, normed, w_out_hbm, give, keep, w_out, sem):
    copy = pltpu.make_async_copy(w_out_hbm, w_out, sem)
    copy.start()
    copy.wait()
    total = dot(normed[...], w_out[...])
    size = give.shape[2]
    first = core[0] == 0
    for y in range(give.shape[0]):
        even = total[:, 2 * y * size : (2 * y + 1) * size]
        odd = total[:, (2 * y + 1) * size : (2 * y + 2) * size]
        keep[y] = jnp.where(first, even, odd)
        give[y] = jnp.where(first, odd, even)


def chip_kernel(y, keep, got, own, *away):
    size = keep.shape[0]
    own[...] = keep[y[0]] + got[y[0]]
    for n, out in enumerate(away):
        at = (y[0] + n + 1) % size
        out[...] = keep[at] + got[at]


def head_exchange(normed, w_out, y_size):
    rows = normed.shape[0]
    heads = 2 * y_size
    size = w_out.shape[1] // heads
    head = lax.axis_index("head")
    in_smem = pl.BlockSpec(memory_space=pltpu.SMEM)
    in_vmem = pl.BlockSpec(memory_space=pltpu.VMEM)
    limit = pltpu.CompilerParams(vmem_limit_bytes=8 * 1024 * 1024)
    piece = jax.ShapeDtypeStruct((y_size, rows, size), jnp.float32)
    give, keep = pl.pallas_call(
        project_kernel,
        in_specs=[in_smem, in_vmem, pl.BlockSpec(memory_space=pl.ANY)],
        out_specs=[in_vmem, in_vmem],
        out_shape=[piece, piece],
        scratch_shapes=[pltpu.VMEM(w_out.shape, w_out.dtype), pltpu.SemaphoreType.DMA],
        compiler_params=limit,
        name="project_out",
    )((head % 2)[None], normed, pltpu.with_memory_space_constraint(w_out, pltpu.HBM))
    got = lax.ppermute(give, "head", [(h, h ^ 1) for h in range(heads)])
    total, *away = pl.pallas_call(
        chip_kernel,
        in_specs=[in_smem, in_vmem, in_vmem],
        out_specs=[in_vmem] * y_size,
        out_shape=[jax.ShapeDtypeStruct((rows, size), jnp.float32)] * y_size,
        compiler_params=limit,
        name="chip_sum",
    )((head // 2)[None], keep, got)
    for s, part in enumerate(away, 1):
        total = total + lax.ppermute(part, "head", [(h, (h + 2 * s) % heads) for h in range(heads)])
    return total


def decode(
    hidden_in,
    w_query,
    w_key,
    w_value,
    w_zgate,
    w_decay,
    w_beta,
    decay_log,
    dt_bias,
    norm_gain,
    w_out,
    state,
):
    parts = lax.axis_size("row")
    seqs, width = hidden_in.shape
    rows = seqs // parts
    heads = state.shape[1]
    key_rows = w_query.shape[1] * w_query.shape[2]
    f32 = jnp.float32

    def in_hbm(value):
        return pltpu.with_memory_space_constraint(value, pltpu.HBM)

    any_space = pl.BlockSpec(memory_space=pl.ANY)
    in_vmem = pl.BlockSpec(memory_space=pltpu.VMEM)
    limit = pltpu.CompilerParams(vmem_limit_bytes=20 * 1024 * 1024)
    extra = heads * rows + SUB
    per_k, per_q = (SIDE, extra, LANES), (SIDE, heads * rows, LANES)
    *sent, keys, decay_all, decay, beta = pl.pallas_call(
        read_kernel,
        in_specs=[any_space] * 8,
        out_specs=[in_vmem] * (2 * SIDE) + [any_space] * 2 + [in_vmem] * 2,
        out_shape=[pltpu.VMEM(per_k, f32)] * SIDE
        + [pltpu.VMEM(per_q, f32)] * SIDE
        + [pltpu.HBM((key_rows, seqs), f32), pltpu.HBM((seqs, heads), f32)]
        + [jax.ShapeDtypeStruct((rows, heads), f32)] * 2,
        scratch_shapes=[
            pltpu.VMEM((seqs // LANES, LANES, width), jnp.bfloat16),
            pltpu.VMEM((LANES, width), jnp.bfloat16),
            pltpu.VMEM((heads, width), jnp.bfloat16),
            pltpu.VMEM((heads, width), jnp.bfloat16),
            pltpu.VMEM((1, heads), f32),
            pltpu.VMEM((1, heads), f32),
            pltpu.VMEM((parts, rows, heads, SUB, LANES), f32),
            pltpu.VMEM((SIDE, *per_k), f32),
            pltpu.VMEM((2 * key_rows // SUB, 2 * LANES // BLOCK, BLOCK, BLOCK * SUB), jnp.bfloat16),
            pltpu.VMEM((2 * key_rows // SUB, LANES, BLOCK * SUB), jnp.bfloat16),
            pltpu.VMEM((SUB, LANES), f32),
            pltpu.VMEM((key_rows, seqs), f32),
            pltpu.VMEM((seqs, heads), f32),
            pltpu.VMEM((seqs, heads), f32),
            pltpu.SemaphoreType.DMA((6,)),
            pltpu.SemaphoreType.DMA((seqs // LANES,)),
            pltpu.SemaphoreType.DMA((parts,)),
            pltpu.SemaphoreType.DMA((SIDE,)),
            pltpu.SemaphoreType.DMA((2,)),
        ],
        compiler_params=limit,
        name="read_state",
    )(
        in_hbm(hidden_in),
        in_hbm(jnp.transpose(w_query, (1, 2, 0)).reshape(key_rows, width)),
        in_hbm(jnp.transpose(w_key, (1, 2, 0)).reshape(key_rows, width)),
        in_hbm(jnp.transpose(w_decay)),
        in_hbm(jnp.transpose(w_beta)),
        in_hbm(decay_log[None]),
        in_hbm(dt_bias[None]),
        in_hbm(state),
    )

    def along_x(value, step):
        return lax.ppermute(value, "row", [(n, (n + SIDE * step) % parts) for n in range(parts)])

    def along_z(value, step):
        return lax.ppermute(value, "row", [(n, n // SIDE * SIDE + (n + step) % SIDE) for n in range(parts)])

    steps = (1, 3, 2)
    pairs = [(along_x(sent[n], n), along_z(sent[SIDE + n], n)) for n in steps]
    got_k, got_q = zip(*pairs)
    part_k, part_q = (
        [(own[n] + got[0][n]) + (got[1][n] + got[2][n]) for n in range(SIDE)]
        for own, got in ((sent[0], got_k), (sent[SIDE], got_q))
    )
    arrived_k = [part_k[0], *(along_z(part_k[n], n) for n in steps)]
    arrived_q = [part_q[0], *(along_x(part_q[n], n) for n in steps)]

    own_hidden = lax.dynamic_slice_in_dim(hidden_in, lax.axis_index("row") * rows, rows, 0)
    values = jnp.einsum("bd,dhv->hbv", own_hidden, w_value, preferred_element_type=f32)
    zgate = jnp.einsum("bd,dhv->hbv", own_hidden, w_zgate, preferred_element_type=f32)

    delta_sent, delta_own = pl.pallas_call(
        delta_kernel,
        in_specs=[in_vmem] * (SIDE + 3),
        out_specs=[any_space, in_vmem],
        out_shape=[
            pltpu.HBM((parts, heads * rows, LANES), f32),
            jax.ShapeDtypeStruct((extra, LANES), f32),
        ],
        scratch_shapes=[
            pltpu.VMEM((heads * rows, LANES), f32),
            pltpu.SemaphoreType.DMA((parts,)),
        ],
        compiler_params=limit,
        name="owner_delta",
    )(*arrived_k, values, decay, beta)
    delta = lax.all_to_all(delta_sent, "row", 0, 0, tiled=True)

    normed = pl.pallas_call(
        norm_kernel,
        in_specs=[in_vmem] * (SIDE + 4),
        out_specs=in_vmem,
        out_shape=jax.ShapeDtypeStruct((rows, heads * LANES), jnp.bfloat16),
        compiler_params=limit,
        name="owner_norm",
    )(*arrived_q, delta_own, zgate, decay, norm_gain[None])

    layer_out = head_exchange(normed, w_out.reshape(heads * LANES, -1), lax.axis_size("head") // 2).astype(jnp.bfloat16)

    new_state = pl.pallas_call(
        update_kernel,
        in_specs=[in_vmem, any_space, any_space, any_space],
        out_specs=any_space,
        out_shape=pltpu.HBM(state.shape, f32),
        scratch_shapes=[
            pltpu.VMEM((key_rows, seqs), f32),
            pltpu.VMEM((seqs, heads), f32),
            pltpu.VMEM((parts, rows, heads * LANES), f32),
            pltpu.VMEM((parts, rows, heads, SUB, LANES), f32),
            pltpu.VMEM((parts, rows, heads, SUB, LANES), f32),
            pltpu.SemaphoreType.DMA((2,)),
            pltpu.SemaphoreType.DMA((parts,)),
            pltpu.SemaphoreType.DMA((parts,)),
        ],
        compiler_params=pltpu.CompilerParams(vmem_limit_bytes=24 * 1024 * 1024),
        name="update_state",
    )(delta, in_hbm(keys), in_hbm(decay_all), in_hbm(state))
    return (layer_out, new_state)


def solution(mesh):
    in_specs = (
        P(),
        P(None, "head", "row"),
        P(None, "head", "row"),
        P(None, "head", None),
        P(None, "head", None),
        P(None, "head"),
        P(None, "head"),
        P("head"),
        P("head"),
        P(),
        P("head", None, None),
        P(None, "head", "row", None),
    )
    out_specs = (P("row", "head"), P(None, "head", "row", None))
    return jax.shard_map(decode, mesh=mesh, in_specs=in_specs, out_specs=out_specs, check_vma=False)
```

```python
import jax
import jax.numpy as jnp
from jax import lax
from jax.experimental import pallas as pl
from jax.experimental.pallas import tpu as pltpu
from jax.sharding import PartitionSpec as P


LANES = 128
SUB = 8
BLOCK = 16
SIDE = 4
KEY_HEADS = 2


def high_low(value):
    high = value.astype(jnp.bfloat16)
    return high, (value - high.astype(jnp.float32)).astype(jnp.bfloat16)


def dot(left, right):
    return jnp.dot(left, right, preferred_element_type=jnp.float32)


def read_kernel(
    hidden_hbm,
    w_query_hbm,
    w_key_hbm,
    w_decay_hbm,
    w_beta_hbm,
    decay_log_hbm,
    dt_bias_hbm,
    state_hbm,
    *rest,
):
    by_x, by_z = rest[0:SIDE], rest[SIDE : 2 * SIDE]
    keys_hbm, decay_hbm, decay_own, beta_own = rest[2 * SIDE : 2 * SIDE + 4]
    hidden, weights, w_decay, w_beta, decay_log, dt_bias, state = rest[2 * SIDE + 4 : 2 * SIDE + 11]
    reads_k, reads_q, left, picks, sums, keys_all, decay_all, beta_all = rest[2 * SIDE + 11 : 2 * SIDE + 19]
    in_sems, hidden_sems, state_sems, k_sems, q_sems, out_sems = rest[2 * SIDE + 19 :]
    me = lax.axis_index("row")
    my_x, my_z = me // SIDE, me % SIDE
    _, rows, heads = state.shape[0:3]
    chunks = hidden.shape[0]
    blocks = LANES // BLOCK
    key_rows = w_query_hbm.shape[0]
    key_heads = key_rows // SUB
    group = heads // key_heads
    few = BLOCK
    span = few * SUB
    pad = weights.dtype.itemsize * SUB

    inputs = [
        pltpu.make_async_copy(w_query_hbm, weights.at[pad : pad + key_rows], in_sems.at[0]),
        pltpu.make_async_copy(w_key_hbm, weights.at[pad + key_rows : pad + 2 * key_rows], in_sems.at[1]),
        pltpu.make_async_copy(w_decay_hbm, w_decay, in_sems.at[2]),
        pltpu.make_async_copy(decay_log_hbm, decay_log, in_sems.at[3]),
        pltpu.make_async_copy(dt_bias_hbm, dt_bias, in_sems.at[4]),
        pltpu.make_async_copy(w_beta_hbm, w_beta, in_sems.at[5]),
    ]
    for copy in inputs:
        copy.start()

    def chunk_of(s):
        return (my_x + s) % SIDE

    def hidden_copy(s):
        at = pl.multiple_of(chunk_of(s) * LANES, LANES)
        return pltpu.make_async_copy(hidden_hbm.at[pl.ds(at, LANES)], hidden.at[s], hidden_sems.at[s])

    def state_copy(n):
        part = chunk_of(n // SIDE) * SIDE + (my_z + n % SIDE) % SIDE
        return pltpu.make_async_copy(state_hbm.at[pl.ds(part * rows, rows)], state.at[n], state_sems.at[n])

    def k_copy(s, to):
        return pltpu.make_async_copy(reads_k.at[s], to, k_sems.at[s])

    def q_copy(s, t):
        return pltpu.make_async_copy(reads_q.at[t, s], by_z[t].at[s], q_sems.at[t, s])

    ahead = 2
    for n in range(ahead):
        hidden_copy(n).start()
    width = weights.shape[1]
    weights[0:pad] = jnp.zeros((pad, width), weights.dtype)
    weights[pad + 2 * key_rows :] = jnp.zeros((LANES - pad - 2 * key_rows, width), weights.dtype)
    sums[...] = jnp.zeros(sums.shape, sums.dtype)
    source = lax.broadcasted_iota(jnp.int32, (LANES, span), 0)
    entry = lax.broadcasted_iota(jnp.int32, (LANES, span), 1) % SUB
    own = lax.broadcasted_iota(jnp.int32, (few, span), 1) // SUB == lax.broadcasted_iota(jnp.int32, (few, span), 0)
    for n in range(2 * key_heads):
        picks[n] = (source == pad + n * SUB + entry).astype(jnp.bfloat16)
    for copy in inputs:
        copy.wait()
    weights[0:heads] = w_decay[...]
    weights[heads : 2 * heads] = w_beta[...]
    for n in range(ahead * SIDE):
        state_copy(n).start()
        if n % SIDE == 1:
            hidden_copy(ahead + n // SIDE).start()

    @pl.loop(0, chunks)
    def _(s):
        chunk = chunk_of(s)
        hidden_copy(s).wait()

        @pl.when(s + ahead < SIDE)
        def _():
            for t in range(SIDE):
                state_copy((s + ahead) * SIDE + t).start()

        projected = lax.dot_general(hidden[s], weights[...], (((1,), (1,)), ((), ())), preferred_element_type=jnp.float32)
        halves = jnp.concatenate(high_low(projected), axis=0)
        for n in range(2 * key_heads):
            wide = dot(halves, picks[n]).reshape(2 * blocks, few, span)
            left[n] = jnp.where(own[None], wide, 0.0).astype(jnp.bfloat16)

        at = pl.multiple_of(chunk * LANES, LANES)
        pre = projected[:, 0:heads] + dt_bias[...]
        soft = jnp.maximum(pre, 0.0) + jnp.log1p(jnp.exp(-jnp.abs(pre)))
        decay_all[pl.ds(at, LANES)] = jnp.exp(-jnp.exp(decay_log[...]) * soft)
        beta_all[pl.ds(at, LANES)] = 1.0 / (1.0 + jnp.exp(-projected[:, heads : 2 * heads]))
        turned = jnp.transpose(projected)
        query = turned[pad : pad + key_rows]
        keys = turned[pad + key_rows : pad + 2 * key_rows]
        keys_all[:, pl.ds(at, LANES)] = keys
        for n, product in enumerate((query * query, keys * keys, query * keys)):
            for g in range(key_heads):
                sums[n * key_heads + g : n * key_heads + g + 1] = jnp.sum(product[g * SUB : (g + 1) * SUB], axis=0, keepdims=True)

        for t in range(SIDE):
            p = (my_z + t) % SIDE
            turn = s * SIDE + t
            state_copy(turn).wait()
            for first in range(0, rows, few):
                block = p * (rows // few) + first // few
                for g in range(key_heads):
                    tiles = [state[turn, first : first + few, g * group + j].reshape(span, LANES) for j in range(group)]
                    state_high, state_low = high_low(jnp.concatenate(tiles, axis=1))
                    high = jnp.concatenate([left[g, block], left[key_heads + g, block]], axis=0)
                    low = jnp.concatenate([left[g, blocks + block], left[key_heads + g, blocks + block]], axis=0)
                    both = dot(jnp.concatenate([high, low], axis=0), state_high)
                    read = both[0 : 2 * few] + both[2 * few :] + dot(high, state_low)
                    for j in range(group):
                        to = (g * group + j) * rows + first
                        lanes = slice(j * LANES, (j + 1) * LANES)
                        reads_k[s, t, to : to + few] = read[few:, lanes]
                        reads_q[t, s, to : to + few] = read[0:few, lanes]
            reads_k[s, t, heads * rows :] = pltpu.roll(sums[...], (LANES - p * rows) % LANES, 1)
        for t in range(SIDE):
            q_copy(s, t).start()
        for k in range(SIDE):

            @pl.when(s == k)
            def _():
                k_copy(s, by_x[k]).start()

    outputs = [
        pltpu.make_async_copy(keys_all, keys_hbm, out_sems.at[0]),
        pltpu.make_async_copy(decay_all, decay_hbm, out_sems.at[1]),
    ]
    for copy in outputs:
        copy.start()

    mine = pl.ds(pl.multiple_of(me * rows, rows), rows)
    decay_own[...] = decay_all[mine]
    beta_own[...] = beta_all[mine]
    for k in range(SIDE):
        k_copy(k, by_x[k]).wait()
        for t in range(SIDE):
            q_copy(k, t).wait()
    for copy in outputs:
        copy.wait()


def arrived_sum(parts):
    return (parts[0][...] + parts[1][...]) + (parts[2][...] + parts[3][...])


def delta_kernel(*refs):
    values, decay, beta, delta_hbm, delta_out, scaled, out_sems = refs[SIDE:]
    rows, heads = decay.shape
    parts = delta_hbm.shape[0]
    read_k = arrived_sum(refs[0:SIDE])
    raw_sums = read_k[heads * rows :]
    delta_out[heads * rows :] = raw_sums
    sums = jnp.transpose(raw_sums)[0:rows]
    group = heads // KEY_HEADS
    key_scale = lax.rsqrt(1.0 + sums[:, KEY_HEADS : 2 * KEY_HEADS])
    for h in range(heads):
        g = h // group
        at = slice(h * rows, (h + 1) * rows)
        ks = key_scale[:, g : g + 1]
        readk = read_k[at] * ks
        delta = beta[:, h : h + 1] * (values[h] - decay[:, h : h + 1] * readk)
        delta_out[at] = delta
        scaled[at] = delta * ks
    outputs = [pltpu.make_async_copy(scaled, delta_hbm.at[n], out_sems.at[n]) for n in range(parts)]
    for copy in outputs:
        copy.start()
    for copy in outputs:
        copy.wait()


def norm_kernel(*refs):
    deltas, zgate, decay, norm_gain, normed_out = refs[SIDE:]
    rows, heads = decay.shape
    read_q = arrived_sum(refs[0:SIDE])
    sums = jnp.transpose(deltas[heads * rows :])[0:rows]
    group = heads // KEY_HEADS
    query_scale = lax.rsqrt(1.0 + sums[:, 0:KEY_HEADS])
    key_scale = lax.rsqrt(1.0 + sums[:, KEY_HEADS : 2 * KEY_HEADS])
    unit_dot = sums[:, 2 * KEY_HEADS : 3 * KEY_HEADS] * query_scale * key_scale
    for h in range(heads):
        g = h // group
        lanes = slice(h * LANES, (h + 1) * LANES)
        at = slice(h * rows, (h + 1) * rows)
        readq = decay[:, h : h + 1] * (read_q[at] * query_scale[:, g : g + 1]) + unit_dot[:, g : g + 1] * deltas[at]
        meansq = jnp.mean(readq * readq, axis=1, keepdims=True)
        z = zgate[h]
        normed = readq * lax.rsqrt(meansq + 0.5) * norm_gain[...] * (z / (1.0 + jnp.exp(-z)))
        normed_out[:, lanes] = normed.astype(jnp.bfloat16)


def update_kernel(delta, keys_hbm, decay_hbm, state_hbm, new_state, keys, decay, wide, state, ready, small_sems, in_sems, out_sems):
    parts, rows, heads = state.shape[0:3]
    key_heads = keys.shape[0] // SUB
    group = heads // key_heads
    few = BLOCK
    span = few * SUB
    per_tile = LANES // rows

    small = [
        pltpu.make_async_copy(decay_hbm, decay, small_sems.at[0]),
        pltpu.make_async_copy(keys_hbm, keys, small_sems.at[1]),
    ]
    for copy in small:
        copy.start()

    def read(n):
        return pltpu.make_async_copy(state_hbm.at[pl.ds(n * rows, rows)], state.at[n], in_sems.at[n])

    def write(n):
        return pltpu.make_async_copy(ready.at[n], new_state.at[pl.ds(n * rows, rows)], out_sems.at[n])

    ahead = 6
    for n in range(ahead):
        read(n).start()
    lane = lax.broadcasted_iota(jnp.int32, (SUB, LANES), 1)
    slot = lax.broadcasted_iota(jnp.int32, (span, LANES), 1)
    own = (slot % few == lax.broadcasted_iota(jnp.int32, (span, LANES), 0) // SUB) & (slot < 3 * few)
    ones = jnp.ones((LANES, LANES), jnp.bfloat16)
    for copy in small:
        copy.wait()

    @pl.loop(0, parts // per_tile)
    def _(n):
        at = pl.multiple_of(n * LANES, LANES)
        some = decay[pl.ds(at, LANES)]
        for h in range(heads):
            spread = jnp.broadcast_to(some[:, h : h + 1], (LANES, LANES)).reshape(per_tile, rows, LANES)
            wide[pl.ds(n * per_tile, per_tile), :, h * LANES : (h + 1) * LANES] = spread

    @pl.loop(0, parts // per_tile)
    def _(tile):
        raw = keys[:, pl.ds(pl.multiple_of(tile * LANES, LANES), LANES)]
        high = raw.astype(jnp.bfloat16).astype(jnp.float32)
        rest = raw - high
        middle = rest.astype(jnp.bfloat16).astype(jnp.float32)
        low = rest - middle
        for n in range(per_tile):
            part = tile * per_tile + n
            read(part).wait()

            @pl.when(part + ahead < parts)
            def _():
                read(part + ahead).start()

            for first in range(0, rows, few):
                back = LANES - n * rows - first
                turned = [pltpu.roll(x, (back + m * few) % LANES, 1) for m, x in enumerate((high, middle, low))]
                packed = jnp.where(lane[0:1] < few, turned[0], jnp.where(lane[0:1] < 2 * few, turned[1], turned[2]))
                for g in range(key_heads):
                    spread = jnp.broadcast_to(packed[None, g * SUB : (g + 1) * SUB], (few, SUB, LANES)).reshape(span, LANES)
                    wide_key = dot(jnp.where(own, spread, 0.0).astype(jnp.bfloat16), ones)
                    for b in range(few):
                        k = wide_key[b * SUB : (b + 1) * SUB]
                        at = first + b
                        for h in range(g * group, (g + 1) * group):
                            row = jnp.broadcast_to(delta[part, h * rows + at : h * rows + at + 1], (SUB, LANES))
                            factor = jnp.broadcast_to(wide[part, at : at + 1, h * LANES : (h + 1) * LANES], (SUB, LANES))
                            ready[part, at, h] = factor * state[part, at, h] + k * row
            write(part).start()

    @pl.loop(0, parts)
    def _(part):
        write(part).wait()


def project_kernel(core, normed, w_out_hbm, give, keep, w_out, sem):
    copy = pltpu.make_async_copy(w_out_hbm, w_out, sem)
    copy.start()
    copy.wait()
    total = dot(normed[...], w_out[...])
    size = give.shape[2]
    first = core[0] == 0
    for y in range(give.shape[0]):
        even = total[:, 2 * y * size : (2 * y + 1) * size]
        odd = total[:, (2 * y + 1) * size : (2 * y + 2) * size]
        keep[y] = jnp.where(first, even, odd)
        give[y] = jnp.where(first, odd, even)


def chip_kernel(y, keep, got, own, *away):
    size = keep.shape[0]
    own[...] = keep[y[0]] + got[y[0]]
    for n, out in enumerate(away):
        at = (y[0] + n + 1) % size
        out[...] = keep[at] + got[at]


def head_exchange(normed, w_out, y_size):
    rows = normed.shape[0]
    heads = 2 * y_size
    size = w_out.shape[1] // heads
    head = lax.axis_index("head")
    in_smem = pl.BlockSpec(memory_space=pltpu.SMEM)
    in_vmem = pl.BlockSpec(memory_space=pltpu.VMEM)
    limit = pltpu.CompilerParams(vmem_limit_bytes=8 * 1024 * 1024)
    piece = jax.ShapeDtypeStruct((y_size, rows, size), jnp.float32)
    give, keep = pl.pallas_call(
        project_kernel,
        in_specs=[in_smem, in_vmem, pl.BlockSpec(memory_space=pl.ANY)],
        out_specs=[in_vmem, in_vmem],
        out_shape=[piece, piece],
        scratch_shapes=[pltpu.VMEM(w_out.shape, w_out.dtype), pltpu.SemaphoreType.DMA],
        compiler_params=limit,
        name="project_out",
    )((head % 2)[None], normed, pltpu.with_memory_space_constraint(w_out, pltpu.HBM))
    got = lax.ppermute(give, "head", [(h, h ^ 1) for h in range(heads)])
    total, *away = pl.pallas_call(
        chip_kernel,
        in_specs=[in_smem, in_vmem, in_vmem],
        out_specs=[in_vmem] * y_size,
        out_shape=[jax.ShapeDtypeStruct((rows, size), jnp.float32)] * y_size,
        compiler_params=limit,
        name="chip_sum",
    )((head // 2)[None], keep, got)
    for s, part in enumerate(away, 1):
        total = total + lax.ppermute(part, "head", [(h, (h + 2 * s) % heads) for h in range(heads)])
    return total


def decode(
    hidden_in,
    w_query,
    w_key,
    w_value,
    w_zgate,
    w_decay,
    w_beta,
    decay_log,
    dt_bias,
    norm_gain,
    w_out,
    state,
):
    parts = lax.axis_size("row")
    seqs, width = hidden_in.shape
    rows = seqs // parts
    heads = state.shape[1]
    key_rows = w_query.shape[1] * w_query.shape[2]
    f32 = jnp.float32

    def in_hbm(value):
        return pltpu.with_memory_space_constraint(value, pltpu.HBM)

    any_space = pl.BlockSpec(memory_space=pl.ANY)
    in_vmem = pl.BlockSpec(memory_space=pltpu.VMEM)
    limit = pltpu.CompilerParams(vmem_limit_bytes=20 * 1024 * 1024)
    extra = heads * rows + SUB
    per_k, per_q = (SIDE, extra, LANES), (SIDE, heads * rows, LANES)
    *sent, keys, decay_all, decay, beta = pl.pallas_call(
        read_kernel,
        in_specs=[any_space] * 8,
        out_specs=[any_space] * (2 * SIDE + 2) + [in_vmem] * 2,
        out_shape=[pltpu.HBM(per_k, f32)] * SIDE
        + [pltpu.HBM(per_q, f32)] * SIDE
        + [pltpu.HBM((key_rows, seqs), f32), pltpu.HBM((seqs, heads), f32)]
        + [jax.ShapeDtypeStruct((rows, heads), f32)] * 2,
        scratch_shapes=[
            pltpu.VMEM((seqs // LANES, LANES, width), jnp.bfloat16),
            pltpu.VMEM((LANES, width), jnp.bfloat16),
            pltpu.VMEM((heads, width), jnp.bfloat16),
            pltpu.VMEM((heads, width), jnp.bfloat16),
            pltpu.VMEM((1, heads), f32),
            pltpu.VMEM((1, heads), f32),
            pltpu.VMEM((parts, rows, heads, SUB, LANES), f32),
            pltpu.VMEM((SIDE, *per_k), f32),
            pltpu.VMEM((SIDE, *per_q), f32),
            pltpu.VMEM((2 * key_rows // SUB, 2 * LANES // BLOCK, BLOCK, BLOCK * SUB), jnp.bfloat16),
            pltpu.VMEM((2 * key_rows // SUB, LANES, BLOCK * SUB), jnp.bfloat16),
            pltpu.VMEM((SUB, LANES), f32),
            pltpu.VMEM((key_rows, seqs), f32),
            pltpu.VMEM((seqs, heads), f32),
            pltpu.VMEM((seqs, heads), f32),
            pltpu.SemaphoreType.DMA((6,)),
            pltpu.SemaphoreType.DMA((seqs // LANES,)),
            pltpu.SemaphoreType.DMA((parts,)),
            pltpu.SemaphoreType.DMA((SIDE,)),
            pltpu.SemaphoreType.DMA((SIDE, SIDE)),
            pltpu.SemaphoreType.DMA((2,)),
        ],
        compiler_params=limit,
        name="read_state",
    )(
        in_hbm(hidden_in),
        in_hbm(jnp.transpose(w_query, (1, 2, 0)).reshape(key_rows, width)),
        in_hbm(jnp.transpose(w_key, (1, 2, 0)).reshape(key_rows, width)),
        in_hbm(jnp.transpose(w_decay)),
        in_hbm(jnp.transpose(w_beta)),
        in_hbm(decay_log[None]),
        in_hbm(dt_bias[None]),
        in_hbm(state),
    )

    def along_x(value, step):
        return lax.ppermute(value, "row", [(n, (n + SIDE * step) % parts) for n in range(parts)])

    def along_z(value, step):
        return lax.ppermute(value, "row", [(n, n // SIDE * SIDE + (n + step) % SIDE) for n in range(parts)])

    steps = (1, 3, 2)
    pairs = [(along_x(sent[n], n), along_z(sent[SIDE + n], n)) for n in steps]
    got_k, got_q = zip(*pairs)
    part_k, part_q = (
        [(own[n] + got[0][n]) + (got[1][n] + got[2][n]) for n in range(SIDE)]
        for own, got in ((sent[0], got_k), (sent[SIDE], got_q))
    )
    arrived_k = [part_k[0], *(along_z(part_k[n], n) for n in steps)]
    arrived_q = [part_q[0], *(along_x(part_q[n], n) for n in steps)]

    own_hidden = lax.dynamic_slice_in_dim(hidden_in, lax.axis_index("row") * rows, rows, 0)
    values = jnp.einsum("bd,dhv->hbv", own_hidden, w_value, preferred_element_type=f32)
    zgate = jnp.einsum("bd,dhv->hbv", own_hidden, w_zgate, preferred_element_type=f32)

    delta_sent, delta_own = pl.pallas_call(
        delta_kernel,
        in_specs=[in_vmem] * (SIDE + 3),
        out_specs=[any_space, in_vmem],
        out_shape=[
            pltpu.HBM((parts, heads * rows, LANES), f32),
            jax.ShapeDtypeStruct((extra, LANES), f32),
        ],
        scratch_shapes=[
            pltpu.VMEM((heads * rows, LANES), f32),
            pltpu.SemaphoreType.DMA((parts,)),
        ],
        compiler_params=limit,
        name="owner_delta",
    )(*arrived_k, values, decay, beta)
    delta = lax.all_to_all(delta_sent, "row", 0, 0, tiled=True)

    normed = pl.pallas_call(
        norm_kernel,
        in_specs=[in_vmem] * (SIDE + 4),
        out_specs=in_vmem,
        out_shape=jax.ShapeDtypeStruct((rows, heads * LANES), jnp.bfloat16),
        compiler_params=limit,
        name="owner_norm",
    )(*arrived_q, delta_own, zgate, decay, norm_gain[None])

    layer_out = head_exchange(normed, w_out.reshape(heads * LANES, -1), lax.axis_size("head") // 2).astype(jnp.bfloat16)

    new_state = pl.pallas_call(
        update_kernel,
        in_specs=[in_vmem, any_space, any_space, any_space],
        out_specs=any_space,
        out_shape=pltpu.HBM(state.shape, f32),
        scratch_shapes=[
            pltpu.VMEM((key_rows, seqs), f32),
            pltpu.VMEM((seqs, heads), f32),
            pltpu.VMEM((parts, rows, heads * LANES), f32),
            pltpu.VMEM((parts, rows, heads, SUB, LANES), f32),
            pltpu.VMEM((parts, rows, heads, SUB, LANES), f32),
            pltpu.SemaphoreType.DMA((2,)),
            pltpu.SemaphoreType.DMA((parts,)),
            pltpu.SemaphoreType.DMA((parts,)),
        ],
        compiler_params=pltpu.CompilerParams(vmem_limit_bytes=24 * 1024 * 1024),
        name="update_state",
    )(delta, in_hbm(keys), in_hbm(decay_all), in_hbm(state))
    return (layer_out, new_state)


def solution(mesh):
    in_specs = (
        P(),
        P(None, "head", "row"),
        P(None, "head", "row"),
        P(None, "head", None),
        P(None, "head", None),
        P(None, "head"),
        P(None, "head"),
        P("head"),
        P("head"),
        P(),
        P("head", None, None),
        P(None, "head", "row", None),
    )
    out_specs = (P("row", "head"), P(None, "head", "row", None))
    return jax.shard_map(decode, mesh=mesh, in_specs=in_specs, out_specs=out_specs, check_vma=False)
```
